32 devices in a mesh: depth: 2 (over x), lat: 16 (over z, y, core).
Axes of the slice: x: 2, y: 2, z: 4, core: 2. Of those that a mesh axis runs over, the one named last changes fastest.
Arguments:
- displacement: float32 [3, 16, 128, 256], P(None, 'depth', 'lat'), may hold values from -6 to 6
- velocity: float32 [3, 16, 128, 256], P(None, 'depth', 'lat'), may hold values from -6 to 6
- inverse_mass: float32 [16, 128, 256], P('depth', 'lat'), may hold values from 0.5 to 2
- material: int32 [16, 128, 256], P('depth', 'lat'), may hold values from 0 to 7
- dilation_table: float32 [8], replicated, may hold values from 0.5 to 2
- shear_table: float32 [8], replicated, may hold values from 0.5 to 2
- stiffness_pair: float32 [2, 24, 24], replicated, may hold values from -1.5 to 3.5, as said below
- impedance: float32 [3], replicated, may hold values from 0.5 to 2
- bedrock_mask: int32 [128, 256], P('lat'), may hold values 0 or 1
- incident: float32 [6, 3, 128, 256], P(None, None, 'lat'), may hold values from -6 to 6
Outputs:
- new_displacement: float32 [3, 16, 128, 256], P(None, 'depth', 'lat')
- new_velocity: float32 [3, 16, 128, 256], P(None, 'depth', 'lat')
The draws below stay inside these ranges and needn't reach their ends.
Inputs may be any that keep to these rules, and one draw needn't show every extreme that they name: `stiffness_pair`: symmetric positive definite.
All inputs are finite; a program needn't handle non-finite values. No bound on the sum of `bedrock_mask` on one device may be relied on, other than what follows from the above.
Results may differ from the reference program's by a relative error of at most 0.00016.
Values sent between devices are 32-bit elements; how exact they have to be, the bound alone decides.
No kernel may reach another device: no remote copies, remote signals or barrier semaphores. Data moves between devices by JAX's collectives and lax.ppermute only.
A program may use at most 64 MiB of HBM per device.

```python
import math
import jax
import jax.numpy as jnp
from jax import lax

NXC = 256
STEPS = 6
NMAT = 8
NZ = 16
NY = 128


def draw_stiffness_pair(key, part):
    factor = jax.random.normal(key, (2, 24, 24), jnp.float32)
    square = jnp.einsum('aij,akj->aik', factor, factor) / 48.0
    return 0.5 * jnp.eye(24, dtype=jnp.float32)[None] + square


def touch_ends(result, stream_key, low, top_value):
    longest = result.shape.index(max(result.shape))
    spots = []
    for shift in (0, 1):
        where = [jax.random.randint(jax.random.fold_in(stream_key, axis), (), 0, length) for axis, length in enumerate(result.shape)]
        where[longest] = (where[longest] + shift) % result.shape[longest]
        spots.append(tuple(where))
    return result.at[spots[0]].set(low).at[spots[1]].set(top_value)


def block_levels(key, dims, shards, least, high):
    def one(dim, shards_of):
        heights = jax.random.uniform(jax.random.fold_in(jax.random.fold_in(key, 6), dim), (shards_of,), jnp.float32, least / len(shards), high / len(shards))
        return jnp.repeat(jnp.exp(heights), dims[dim] // shards_of).reshape((-1,) + (1,) * (len(dims) - dim - 1))

    loudness = one(*shards[0])
    for cut in shards[1:]:
        loudness = loudness * one(*cut)
    return loudness


def noise(own_key, dims, width, most, shards=(), held_as=jnp.bfloat16):
    drawn = jax.random.normal(own_key, dims, jnp.float32) * width
    if len(shards) > 0:
        drawn = block_levels(own_key, dims, shards, -0.22, 0.18) * drawn
    return jnp.clip(drawn, min=-most, max=most).astype(held_as)


def setup_inputs(seed: int = 0) -> dict:
    key_of = jax.random.split(jax.random.key(seed), 11)
    return {
        "displacement": noise(key_of[0], (3, NZ, NY, NXC), 1.0, 6.0, ((1, 2), (2, 16)), jnp.float32),
        "velocity": noise(key_of[1], (3, NZ, NY, NXC), 1.0, 6.0, ((1, 2), (2, 16)), jnp.float32),
        "inverse_mass": jnp.clip(jnp.exp(math.log(2.0) - 1.3862944 * jax.random.uniform(key_of[2], (NZ, NY, NXC), jnp.float32) ** block_levels(key_of[2], (NZ, NY, NXC), ((0, 2), (1, 16)), -0.2, 0.2)), 0.5, 2.0),
        "material": touch_ends(jax.random.randint(key_of[3], (NZ, NY, NXC), 0, NMAT), jax.random.fold_in(key_of[3], 1), 0, NMAT - 1).astype(jnp.int32),
        "dilation_table": jnp.clip(jnp.exp(jax.random.uniform(key_of[4], (NMAT,), jnp.float32, math.log(0.5), math.log(2.0))), 0.5, 2.0),
        "shear_table": jnp.clip(jnp.exp(jax.random.uniform(key_of[5], (NMAT,), jnp.float32, math.log(0.5), math.log(2.0))), 0.5, 2.0),
        "stiffness_pair": draw_stiffness_pair(jax.random.fold_in(key_of[10], 71), 0),
        "impedance": jnp.clip(jnp.exp(jax.random.uniform(key_of[7], (3,), jnp.float32, math.log(0.5), math.log(2.0))), 0.5, 2.0),
        "bedrock_mask": touch_ends((jax.random.randint(key_of[8], (NY, NXC), 0, 2) < 1).astype(jnp.int32), jax.random.fold_in(key_of[8], 1), 0, 1),
        "incident": noise(key_of[9], (STEPS, 3, NY, NXC), 1.0, 6.0, ((2, 16),), jnp.float32),
    }


time_step = 0.1
highest = lax.Precision.HIGHEST


def layer_forces(lower_plane, upper_plane, dilation_layer, shear_layer, stiffness_rows):
    rows_y, cells_x = dilation_layer.shape
    corners = []
    for node_plane in (lower_plane, upper_plane):
        for shift_y in (0, 1):
            for shift_x in (0, 1):
                corners.append(node_plane[:, shift_y:shift_y + rows_y, shift_x:shift_x + cells_x])
    values = jnp.stack(corners).reshape(24, rows_y * cells_x)
    products = jnp.dot(stiffness_rows, values, precision=highest).reshape(2, 8, 3, rows_y, cells_x)
    element_force = dilation_layer * products[0] + shear_layer * products[1]
    sides = [jnp.zeros((3, rows_y + 1, cells_x + 1), jnp.float32), jnp.zeros((3, rows_y + 1, cells_x + 1), jnp.float32)]
    corner = 0
    for side in range(2):
        for shift_y in (0, 1):
            for shift_x in (0, 1):
                contribution = jnp.pad(element_force[corner], ((0, 0), (shift_y, 1 - shift_y), (shift_x, 1 - shift_x)))
                sides[side] = sides[side] + contribution
                corner += 1
    return sides[0], sides[1]


def assemble(displacement, dilation_field, shear_field, stiffness_rows):
    padded = jnp.pad(displacement, ((0, 0), (0, 1), (0, 1), (0, 1)))
    planes = jnp.moveaxis(padded, 1, 0)

    def advance(carried, inputs):
        lower_plane, upper_plane, dilation_layer, shear_layer = inputs
        low_part, high_part = layer_forces(lower_plane, upper_plane, dilation_layer, shear_layer, stiffness_rows)
        return high_part, carried + low_part

    initial = jnp.zeros(planes.shape[1:], jnp.float32)
    unused, layers = lax.scan(advance, initial, (planes[:-1], planes[1:], dilation_field, shear_field))
    return jnp.moveaxis(layers, 0, 1)[:, :, :-1, :-1]


def reference(displacement, velocity, inverse_mass, material, dilation_table, shear_table, stiffness_pair, impedance, bedrock_mask, incident):
    dilation_field = dilation_table[material]
    shear_field = shear_table[material]
    stiffness_rows = stiffness_pair.reshape(48, 24)
    mask_value = bedrock_mask.astype(jnp.float32)
    bottom = NZ - 1
    for instant in range(STEPS):
        forces = assemble(displacement, dilation_field, shear_field, stiffness_rows)
        traction = impedance[:, None, None] * (2.0 * mask_value * incident[instant] - velocity[:, bottom])
        net_force = (-forces).at[:, bottom].add(traction)
        velocity = velocity + time_step * inverse_mass[None] * net_force
        displacement = displacement + time_step * velocity
    return displacement, velocity
```

```python
import jax
import jax.numpy as jnp
import numpy as np
from jax import lax
from jax.experimental import pallas as pl
from jax.experimental.pallas import tpu as pltpu
from jax.sharding import PartitionSpec as P

time_step = 0.1
LANES = 128
f32 = jnp.float32
bf16 = jnp.bfloat16


class Plan:
    def __init__(self, mesh, displacement, incident):
        self.D = mesh.shape["depth"]
        self.L = mesh.shape["lat"]
        self.Z = displacement.shape[1] // self.D
        self.Y = displacement.shape[2] // self.L
        self.X = displacement.shape[3]
        self.H = self.X // LANES
        self.T = incident.shape[0]
        T = self.T
        assert T <= self.Z and T <= self.Y and self.Y % 8 == 0
        assert self.X % LANES == 0
        self.hy = T + T % 2
        self.YB = self.Y + 2 * self.hy
        self.PB = self.YB // 2
        self.P0 = self.hy // 2
        self.swap = self.D == 2
        self.ZB = self.Z + (0 if self.D == 1 else T if self.swap else 2 * T)
        self.ZS = self.ZB + 2
        self.YL = -(-self.YB // 8) * 8
        self.gpairs = [-(-(T - 1 - s) // 2) for s in range(T)]
        self.grows = 8 * sum(self.gpairs)
        self.hrow = 4 * self.hy
        self.GL = -(-self.grows // (2 * self.hrow))

    def offset(self, depth):
        if self.D == 1:
            return 0
        return depth * self.T if self.swap else self.T


def g_slots(plan):
    slots, g = [], 0
    for s, n in enumerate(plan.gpairs):
        for k in range(n):
            slots.append((s, k, n, plan.ZB + (8 * g) // (2 * plan.hrow), (8 * g) % (2 * plan.hrow)))
            g += 1
    return slots


def selectors():
    rows = np.zeros((4, 64, 48), np.float32)
    cols = np.zeros((2, 4, 24, 256), np.float32)

    def half(parity, dx):
        return 4 * (dx ^ parity)

    blocks = [(0, 0, 0), (8, 0, 0), (16, 0, 1), (24, 1, 1), (32, 1, 0), (40, 1, 0), (48, 2, 0), (56, 2, 0), (64, 2, 1)]
    for ez in range(2):
        for ey in range(2):
            e = 2 * ez + ey
            for lm in range(2):
                for dz in range(2):
                    for dy in range(2):
                        for dx in range(2):
                            for c in range(3):
                                dof = (4 * dz + 2 * dy + dx) * 3 + c
                                r = half((ey + dy) % 2, dx) + c
                                rows[e, ((lm * 2 + dz) * 2 + dy) * 8 + r, lm * 24 + dof] = 1
            for base, node, low in blocks:
                for zn in range(3):
                    dz, dy = zn - ez, node - ey
                    if dz in (0, 1) and dy in (0, 1):
                        for dx in range(2):
                            for c in range(3):
                                dof = (4 * dz + 2 * dy + dx) * 3 + c
                                cols[low, e, dof, zn * 80 + base + half(node % 2, dx) + c] = 1
    return rows, cols


def matrix_kernel(stiff_ref, rows_ref, cols_ref, out_ref):
    stiff = stiff_ref[...]
    high = stiff.astype(bf16)
    low = (stiff - high.astype(f32)).astype(bf16)
    for e in range(4):
        total = None
        for part, k in ((high, 0), (low, 1)):
            picked = jnp.dot(rows_ref[e], part, preferred_element_type=f32).astype(bf16)
            placed = jnp.dot(picked, cols_ref[k, e], preferred_element_type=f32)
            total = placed if total is None else total + placed
        out_ref[64 * e : 64 * e + 64, :] = total.astype(bf16)


def pack_kernel(plan, scal, u, v, m, mat, mask, inc, xv, g, *zsends):
    Z, Y, H, T = plan.Z, plan.Y, plan.H, plan.T
    for z in range(Z):
        for h in range(H):
            lanes = slice(h * LANES, (h + 1) * LANES)
            for y in range(0, Y, 8):
                rows = slice(y, y + 8)
                for c in range(3):
                    xv[z, h, pl.ds(4 * y + c, 8, stride=4), :] = u[c, z, rows, lanes]
                    xv[z, h, pl.ds(4 * (Y + y) + c, 8, stride=4), :] = v[c, z, rows, lanes]
                xv[z, h, pl.ds(4 * y + 3, 8, stride=4), :] = mat[z, rows, lanes].astype(f32) + 1.0
                xv[z, h, pl.ds(4 * (Y + y) + 3, 8, stride=4), :] = m[z, rows, lanes]
    for h in range(H):
        lanes = slice(h * LANES, (h + 1) * LANES)
        for y in range(0, Y, 8):
            rows = slice(y, y + 8)
            double = 2.0 * mask[rows, lanes].astype(f32)
            for s in range(T):
                for c in range(3):
                    g[s, h, pl.ds(4 * y + c, 8, stride=4), :] = double * inc[s, c, rows, lanes]
                g[s, h, pl.ds(4 * y + 3, 8, stride=4), :] = jnp.zeros((8, LANES), f32)
    for k, zsend in enumerate(zsends):
        if plan.swap:
            first = jnp.where(scal[0] == 0, Z - T, 0)
            first_v = jnp.where(scal[0] == 0, Z - T + 1, 0)
        else:
            first, first_v = (Z - T, Z - T + 1) if k == 0 else (0, 0)
        for i in range(T):
            zsend[i] = xv[first + i, :, : 4 * Y, :]
        for i in range(T - 1):
            zsend[T + i] = xv[first_v + i, :, 4 * Y :, :]


def halo_places(plan, scal):
    if plan.D == 1:
        return []
    if plan.swap:
        top = scal[0] == 0
        return [
            (
                jnp.where(top, plan.Z, 0),
                jnp.where(top, plan.Z, 1),
                jnp.where(top, plan.Z + plan.T - 1, 0),
            )
        ]
    last = plan.T + plan.Z
    return [(0, 1, 0), (last, last, last + plan.T - 1)]


def edge_kernel(plan, scal, xv, g, *refs):
    n = len(refs) - 2
    zrecvs, to_prev, to_next = refs[:n], refs[n], refs[n + 1]
    Y, T, R = plan.Y, plan.T, plan.hrow
    offset = scal[1]
    sides = ((to_prev, 0), (to_next, 4 * Y - R))
    for z in range(plan.Z):
        for out, row in sides:
            out[offset + z, :, :R, :] = xv[z, :, row : row + R, :]
            out[offset + z, :, R:, :] = xv[z, :, 4 * Y + row : 4 * Y + row + R, :]
    for zrecv, (at_u, at_v, lacks) in zip(zrecvs, halo_places(plan, scal)):
        for out, row in sides:
            for i in range(T):
                out[at_u + i, :, :R, :] = zrecv[i, :, row : row + R, :]
            for i in range(T - 1):
                out[at_v + i, :, R:, :] = zrecv[T + i, :, row : row + R, :]
            out[lacks, :, R:, :] = jnp.zeros((plan.H, R, LANES), f32)
    for s, k, n_pairs, layer, row in g_slots(plan):
        to_prev[layer, :, row : row + 8, :] = g[s, :, 8 * k : 8 * k + 8, :]
        at = 4 * Y - 8 * n_pairs + 8 * k
        to_next[layer, :, row : row + 8, :] = g[s, :, at : at + 8, :]


def main_kernel(plan, scal, tables, imp, weights, xv, gown, *refs):
    n = len(refs) - 2 - 2 - 9
    zrecvs = refs[:n]
    from_prev, from_next, out_u, out_v = refs[n : n + 4]
    U, V, DM, lam, mu, G, CI, F, KB = refs[n + 4 :]
    Z, Y, X, H, T = plan.Z, plan.Y, plan.X, plan.H, plan.T
    PB, P0, R, ZB, ZS, YB = plan.PB, plan.P0, plan.hrow, plan.ZB, plan.ZS, plan.YB
    offset = scal[1]
    halves = range(H)
    row = lax.broadcasted_iota(jnp.int32, (8, LANES), 0)
    lane = lax.broadcasted_iota(jnp.int32, (8, LANES), 1)
    first_half = row < 4
    spare = (row == 3) | (row == 7)
    zero = jnp.zeros((8, LANES), f32)

    def shift_left(parts):
        rolled = [pltpu.roll(p, LANES - 1, 1) for p in parts] + [zero]
        return [jnp.where(lane == LANES - 1, rolled[h + 1], rolled[h]) for h in halves]

    def shift_right(parts):
        rolled = [zero] + [pltpu.roll(p, 1, 1) for p in parts]
        return [jnp.where(lane == 0, rolled[h], rolled[h + 1]) for h in halves]

    def columns(parts):
        ahead = shift_left(parts)
        tiles = []
        for h in halves:
            swapped = pltpu.roll(ahead[h], 4, 0)
            even = jnp.where(first_half, parts[h], swapped)
            odd = jnp.where(first_half, swapped, parts[h])
            high0 = even.astype(bf16).astype(f32)
            high1 = odd.astype(bf16).astype(f32)
            tiles.append(
                (
                    jnp.concatenate([high0, even - high0], 0).astype(bf16),
                    jnp.concatenate([high0, high1], 0).astype(bf16),
                    jnp.concatenate([high1, odd - high1], 0).astype(bf16),
                )
            )
        return tiles

    def put_columns(buffers, z, p, parts):
        for h, tiles in enumerate(columns(parts)):
            for j in range(3):
                for b in buffers:
                    KB[b, z, p, 16 * j : 16 * j + 16, h * LANES : (h + 1) * LANES] = tiles[j]

    mid = slice(R, R + 4 * Y)
    for z in range(Z):
        U[offset + z, :, mid, :] = xv[z, :, : 4 * Y, :]
        V[offset + z, :, mid, :] = xv[z, :, 4 * Y :, :]
    for zrecv, (at_u, at_v, lacks) in zip(zrecvs, halo_places(plan, scal)):
        for i in range(T):
            U[at_u + i, :, mid, :] = zrecv[i]
        for i in range(T - 1):
            V[at_v + i, :, mid, :] = zrecv[T + i]
        V[lacks, :, mid, :] = jnp.zeros((H, 4 * Y, LANES), f32)
    U[ZB:, :, :, :] = jnp.zeros((ZS - ZB, H, 4 * YB, LANES), f32)
    V[ZB:, :, :, :] = jnp.zeros((ZS - ZB, H, 4 * YB, LANES), f32)
    for s in range(T):
        G[s] = jnp.zeros((H, 4 * YB, LANES), f32)
        G[s, :, mid, :] = gown[s]
    for s, k, n_pairs, layer, at in g_slots(plan):
        low = R - 8 * n_pairs + 8 * k
        G[s, :, low : low + 8, :] = from_prev[layer, :, at : at + 8, :]
        high = R + 4 * Y + 8 * k
        G[s, :, high : high + 8, :] = from_next[layer, :, at : at + 8, :]

    def begin(z, carry):
        for source, here in ((from_prev, slice(0, R)), (from_next, slice(R + 4 * Y, 4 * YB))):
            U[z, :, here, :] = source[z, :, :R, :]
            V[z, :, here, :] = source[z, :, R:, :]
        return carry

    lax.fori_loop(0, ZB, begin, 0)

    n_levels = tables.shape[1]

    def prepare(z, carry):
        for h in halves:
            for y in range(0, plan.YL, 8):
                count = min(8, YB - y)
                if count == 8:
                    level = U[z, h, pl.ds(4 * y + 3, 8, stride=4), :]
                    first = y
                else:
                    first = YB - 8
                    level = U[z, h, pl.ds(4 * first + 3, 8, stride=4), :]
                dil = jnp.zeros((8, LANES), f32)
                she = jnp.zeros((8, LANES), f32)
                for k in range(n_levels):
                    here = level == float(k + 1)
                    dil = jnp.where(here, tables[0, k], dil)
                    she = jnp.where(here, tables[1, k], she)
                lam[z, h, first : first + 8, :] = dil
                mu[z, h, first : first + 8, :] = she
        for p in range(PB):
            at = slice(8 * p, 8 * p + 8)
            for h in halves:
                v = V[z, h, at, :]
                mass = jnp.where(
                    first_half,
                    jnp.broadcast_to(v[3:4, :], (8, LANES)),
                    jnp.broadcast_to(v[7:8, :], (8, LANES)),
                )
                DM[z, h, at, :] = jnp.where(spare, 0.0, time_step * mass)
            put_columns((0, 1), z, p, [U[z, h, at, :] for h in halves])
        for b in range(2):
            KB[b, z, PB] = jnp.zeros((48, X), bf16)
        return carry

    lax.fori_loop(0, ZS, prepare, 0)

    bottom = offset + Z - 1
    wave = jnp.zeros((8, LANES), f32)
    for c in range(3):
        wave = jnp.where((row == c) | (row == 4 + c), imp[c], wave)
    wave = jnp.where(scal[2] == 1, wave, zero)
    for h in halves:
        for p in range(PB):
            at = slice(8 * p, 8 * p + 8)
            CI[h, at, :] = wave * DM[bottom, h, at, :]

    def one_step(s, final):
        d = T - 1 - s
        cur, new = s % 2, 1 - s % 2
        p_first = (plan.hy - d - 1) // 2
        p_last = (plan.hy + Y - 1 + d) // 2
        if plan.D == 1:
            p_z0, count = 0, -(-Z // 2)
        elif plan.swap:
            top = scal[0] == 0
            n_low = -(-(Z + d + 1) // 2)
            count = jnp.where(top, -(-(Z + d) // 2), n_low)
            p_z0 = jnp.where(top, 0, ZB - 2 * n_low)
        else:
            p_z0 = T - d - 1
            count = -(-(Z + 2 * d + 1) // 2)

        for p in range(p_first, p_last + 1):
            at = slice(8 * p, 8 * p + 8)
            for h in halves:
                v = V[bottom, h, at, :]
                V[bottom, h, at, :] = v + CI[h, at, :] * (G[s, h, at, :] - v)
        for p in range(p_first, p_last + 1):
            F[p] = jnp.zeros((2, H, 8, LANES), f32)

        def finish(z, p, g0, g1):
            at = slice(8 * p, 8 * p + 8)
            other = [
                pltpu.roll(jnp.where(first_half, g1[h], g0[h]), 4, 0) for h in halves
            ]
            other = shift_right(other)
            fresh = []
            for h in halves:
                force = jnp.where(first_half, g0[h], g1[h]) + other[h]
                v = V[z, h, at, :] - DM[z, h, at, :] * force
                u = U[z, h, at, :] + time_step * v
                V[z, h, at, :] = v
                U[z, h, at, :] = u
                fresh.append(u)
            if not final:
                put_columns((new,), z, p, fresh)

        def two_layers(i, carry):
            z0 = p_z0 + 2 * i
            side = [[zero for _ in halves] for _ in range(3)]
            for p in range(p_first, p_last + 1):
                right = jnp.concatenate(
                    [
                        KB[cur, z0, p],
                        KB[cur, z0, p + 1, :32],
                        KB[cur, z0 + 1, p],
                        KB[cur, z0 + 1, p + 1, :32],
                        KB[cur, z0 + 2, p],
                        KB[cur, z0 + 2, p + 1],
                    ],
                    0,
                )
                product = jnp.dot(weights[...], right, preferred_element_type=f32)
                node = [[None] * 3 for _ in range(3)]
                for zn in range(3):
                    node[zn][0] = side[zn]
                for y in range(2):
                    above = [F[p, y, h] for h in halves]
                    node[0][y] = above if y else [a + b for a, b in zip(node[0][0], above)]
                for ez in range(2):
                    for ey in range(2):
                        base = 64 * (2 * ez + ey)
                        y = 2 * p + ey
                        for h in halves:
                            lanes = slice(h * LANES, (h + 1) * LANES)
                            dil = jnp.broadcast_to(lam[z0 + ez, h, y : y + 1, :], (8, LANES))
                            she = jnp.broadcast_to(mu[z0 + ez, h, y : y + 1, :], (8, LANES))
                            for dz in range(2):
                                for dy in range(2):
                                    r = base + 8 * (2 * dz + dy)
                                    part = (
                                        dil * product[r : r + 8, lanes]
                                        + she * product[r + 32 : r + 40, lanes]
                                    )
                                    slot = node[ez + dz][ey + dy]
                                    if slot is None:
                                        slot = node[ez + dz][ey + dy] = [None] * H
                                    elif slot is side[ez + dz]:
                                        slot = node[ez + dz][ey + dy] = list(slot)
                                    slot[h] = part if slot[h] is None else slot[h] + part
                for y in range(2):
                    for h in halves:
                        F[p, y, h] = node[2][y][h]
                finish(z0, p, node[0][0], node[0][1])
                finish(z0 + 1, p, node[1][0], node[1][1])
                side = [node[zn][2] for zn in range(3)]
            return carry

        lax.fori_loop(0, count, two_layers, 0)

    for s in range(T):
        one_step(s, s == T - 1)

    for z in range(Z):
        for h in halves:
            lanes = slice(h * LANES, (h + 1) * LANES)
            for y in range(0, Y, 8):
                for c in range(3):
                    at = pl.ds(R + 4 * y + c, 8, stride=4)
                    out_u[c, z, y : y + 8, lanes] = U[offset + z, h, at, :]
                    out_v[c, z, y : y + 8, lanes] = V[offset + z, h, at, :]


def smem():
    return pl.BlockSpec(memory_space=pltpu.SMEM)


def vmem():
    return pl.BlockSpec(memory_space=pltpu.VMEM)


def per_device(plan, u, v, m, mat, dilation_table, shear_table, stiffness_pair, impedance, mask, inc):
    Z, Y, X, H, T, D, L = plan.Z, plan.Y, plan.X, plan.H, plan.T, plan.D, plan.L
    depth = lax.axis_index("depth")
    scal = jnp.stack(
        [depth, jnp.asarray(plan.offset(depth)), (depth == D - 1).astype(jnp.int32)]
    ).astype(jnp.int32)
    shape = lambda *dims: jax.ShapeDtypeStruct(dims, f32)

    rows, cols = selectors()
    weights = pl.pallas_call(
        matrix_kernel,
        out_shape=jax.ShapeDtypeStruct((256, 256), bf16),
        name="matrix",
    )(stiffness_pair.reshape(48, 24), jnp.asarray(rows, bf16), jnp.asarray(cols, bf16))

    n_sends = 0 if D == 1 else 1 if plan.swap else 2
    packed = pl.pallas_call(
        lambda *refs: pack_kernel(plan, *refs),
        out_shape=[shape(Z, H, 8 * Y, LANES), shape(T, H, 4 * Y, LANES)]
        + [shape(2 * T - 1, H, 4 * Y, LANES)] * n_sends,
        in_specs=[smem()] + [vmem()] * 6,
        out_specs=[vmem()] * (2 + n_sends),
        name="pack",
    )(scal, u, v, m, mat, mask, inc)
    xv, g, sends = packed[0], packed[1], packed[2:]
    if D == 1:
        zrecvs = []
    elif plan.swap:
        zrecvs = [lax.ppermute(sends[0], "depth", [(0, 1), (1, 0)])]
    else:
        zrecvs = [
            lax.ppermute(sends[0], "depth", [(i, i + 1) for i in range(D - 1)]),
            lax.ppermute(sends[1], "depth", [(i + 1, i) for i in range(D - 1)]),
        ]
    edge = shape(plan.ZB + plan.GL, H, 2 * plan.hrow, LANES)
    to_prev, to_next = pl.pallas_call(
        lambda *refs: edge_kernel(plan, *refs),
        out_shape=[edge, edge],
        in_specs=[smem()] + [vmem()] * (2 + len(zrecvs)),
        out_specs=[vmem()] * 2,
        name="edge",
    )(scal, xv, g, *zrecvs)
    from_next = lax.ppermute(to_prev, "lat", [(i + 1, i) for i in range(L - 1)])
    from_prev = lax.ppermute(to_next, "lat", [(i, i + 1) for i in range(L - 1)])
    tables = jnp.stack([dilation_table, shear_table])
    grid = (plan.ZS, H, 4 * plan.YB, LANES)
    new_u, new_v = pl.pallas_call(
        lambda *refs: main_kernel(plan, *refs),
        out_shape=[shape(3, Z, Y, X)] * 2,
        in_specs=[smem()] * 3 + [vmem()] * (5 + len(zrecvs)),
        out_specs=[vmem()] * 2,
        scratch_shapes=[
            pltpu.VMEM(grid, f32),
            pltpu.VMEM(grid, f32),
            pltpu.VMEM(grid, f32),
            pltpu.VMEM((plan.ZS, H, plan.YL, LANES), f32),
            pltpu.VMEM((plan.ZS, H, plan.YL, LANES), f32),
            pltpu.VMEM((T, H, 4 * plan.YB, LANES), f32),
            pltpu.VMEM((H, 4 * plan.YB, LANES), f32),
            pltpu.VMEM((plan.PB, 2, H, 8, LANES), f32),
            pltpu.VMEM((2, plan.ZS, plan.PB + 1, 48, X), bf16),
        ],
        name="steps",
    )(scal, tables, impedance, weights, xv, g, *zrecvs, from_prev, from_next)
    return new_u, new_v


def solution(mesh):
    field = P(None, "depth", "lat", None)
    in_specs = (
        field,
        field,
        P("depth", "lat", None),
        P("depth", "lat", None),
        P(),
        P(),
        P(),
        P(),
        P("lat", None),
        P(None, None, "lat", None),
    )

    def whole(displacement, *rest):
        plan = Plan(mesh, displacement, rest[-1])
        return jax.shard_map(
            lambda *args: per_device(plan, *args),
            mesh=mesh,
            in_specs=in_specs,
            out_specs=(field, field),
            check_vma=False,
        )(displacement, *rest)

    return whole
```

```python
import jax
import jax.numpy as jnp
import numpy as np
from jax import lax
from jax.experimental import pallas as pl
from jax.experimental.pallas import tpu as pltpu
from jax.sharding import PartitionSpec as P

time_step = 0.1
LANES = 128
f32 = jnp.float32
bf16 = jnp.bfloat16


class Plan:
    def __init__(self, mesh, displacement, incident):
        self.D = mesh.shape["depth"]
        self.L = mesh.shape["lat"]
        self.Z = displacement.shape[1] // self.D
        self.Y = displacement.shape[2] // self.L
        self.X = displacement.shape[3]
        self.H = self.X // LANES
        self.T = incident.shape[0]
        T = self.T
        assert T <= self.Z and T <= self.Y and self.Y % 8 == 0
        assert self.X % LANES == 0
        self.hy = T + T % 2
        self.YB = self.Y + 2 * self.hy
        self.PB = self.YB // 2
        self.P0 = self.hy // 2
        self.swap = self.D == 2
        self.ZB = self.Z + (0 if self.D == 1 else T if self.swap else 2 * T)
        self.ZS = self.ZB + 2
        self.YL = -(-self.YB // 8) * 8
        self.gpairs = [-(-(T - 1 - s) // 2) for s in range(T)]
        self.hrow = 4 * self.hy

    def offset(self, depth):
        if self.D == 1:
            return 0
        return depth * self.T if self.swap else self.T

    def own_tiles(self):
        n = self.hy // 2
        tiles = [(f, z, h, p) for f in (0, 1) for z in range(self.Z) for h in range(self.H) for p in range(n)]
        waves = [
            (s, h, k, n_pairs)
            for s, n_pairs in enumerate(self.gpairs)
            for h in range(self.H)
            for k in range(n_pairs)
        ]
        return tiles, waves

    def corner_tiles(self):
        n = self.hy // 2
        return [(i, h, p) for i in range(2 * self.T - 1) for h in range(self.H) for p in range(n)]


def selectors():
    rows = np.zeros((4, 64, 48), np.float32)
    cols = np.zeros((2, 4, 24, 256), np.float32)

    def half(parity, dx):
        return 4 * (dx ^ parity)

    blocks = [(0, 0, 0), (8, 0, 0), (16, 0, 1), (24, 1, 1), (32, 1, 0), (40, 1, 0), (48, 2, 0), (56, 2, 0), (64, 2, 1)]
    for ez in range(2):
        for ey in range(2):
            e = 2 * ez + ey
            for lm in range(2):
                for dz in range(2):
                    for dy in range(2):
                        for dx in range(2):
                            for c in range(3):
                                dof = (4 * dz + 2 * dy + dx) * 3 + c
                                r = half((ey + dy) % 2, dx) + c
                                rows[e, ((lm * 2 + dz) * 2 + dy) * 8 + r, lm * 24 + dof] = 1
            for base, node, low in blocks:
                for zn in range(3):
                    dz, dy = zn - ez, node - ey
                    if dz in (0, 1) and dy in (0, 1):
                        for dx in range(2):
                            for c in range(3):
                                dof = (4 * dz + 2 * dy + dx) * 3 + c
                                cols[low, e, dof, zn * 80 + base + half(node % 2, dx) + c] = 1
    return rows, cols


def matrix_kernel(stiff_ref, rows_ref, cols_ref, out_ref):
    stiff = stiff_ref[...]
    high = stiff.astype(bf16)
    low = (stiff - high.astype(f32)).astype(bf16)
    for e in range(4):
        total = None
        for part, k in ((high, 0), (low, 1)):
            picked = jnp.dot(rows_ref[e], part, preferred_element_type=f32).astype(bf16)
            placed = jnp.dot(picked, cols_ref[k, e], preferred_element_type=f32)
            total = placed if total is None else total + placed
        out_ref[64 * e : 64 * e + 64, :] = total.astype(bf16)


def pack_kernel(plan, scal, u, v, m, mat, mask, inc, xv, g, to_prev, to_next, *zsends):
    Z, Y, H, T = plan.Z, plan.Y, plan.H, plan.T
    for z in range(Z):
        for h in range(H):
            lanes = slice(h * LANES, (h + 1) * LANES)
            for y in range(0, Y, 8):
                rows = slice(y, y + 8)
                for c in range(3):
                    xv[z, h, pl.ds(4 * y + c, 8, stride=4), :] = u[c, z, rows, lanes]
                    xv[z, h, pl.ds(4 * (Y + y) + c, 8, stride=4), :] = v[c, z, rows, lanes]
                xv[z, h, pl.ds(4 * y + 3, 8, stride=4), :] = mat[z, rows, lanes].astype(f32) + 1.0
                xv[z, h, pl.ds(4 * (Y + y) + 3, 8, stride=4), :] = m[z, rows, lanes]
    for h in range(H):
        lanes = slice(h * LANES, (h + 1) * LANES)
        for y in range(0, Y, 8):
            rows = slice(y, y + 8)
            double = 2.0 * mask[rows, lanes].astype(f32)
            for s in range(T):
                for c in range(3):
                    g[s, h, pl.ds(4 * y + c, 8, stride=4), :] = double * inc[s, c, rows, lanes]
                g[s, h, pl.ds(4 * y + 3, 8, stride=4), :] = jnp.zeros((8, LANES), f32)
    tiles, waves = plan.own_tiles()
    for out, low in ((to_prev, 0), (to_next, 4 * Y - plan.hrow)):
        for t, (f, z, h, p) in enumerate(tiles):
            at = 4 * Y * f + low + 8 * p
            out[t] = xv[z, h, at : at + 8, :]
        for t, (s, h, k, n_pairs) in enumerate(waves):
            at = 8 * k if low == 0 else 4 * Y - 8 * n_pairs + 8 * k
            out[len(tiles) + t] = g[s, h, at : at + 8, :]
    for k, zsend in enumerate(zsends):
        if plan.swap:
            first = jnp.where(scal[0] == 0, Z - T, 0)
            first_v = jnp.where(scal[0] == 0, Z - T + 1, 0)
        else:
            first, first_v = (Z - T, Z - T + 1) if k == 0 else (0, 0)
        for i in range(T):
            zsend[i] = xv[first + i, :, : 4 * Y, :]
        for i in range(T - 1):
            zsend[T + i] = xv[first_v + i, :, 4 * Y :, :]


def halo_places(plan, scal):
    if plan.D == 1:
        return []
    if plan.swap:
        top = scal[0] == 0
        return [
            (
                jnp.where(top, plan.Z, 0),
                jnp.where(top, plan.Z, 1),
                jnp.where(top, plan.Z + plan.T - 1, 0),
            )
        ]
    last = plan.T + plan.Z
    return [(0, 1, 0), (last, last, last + plan.T - 1)]


def corner_kernel(plan, *refs):
    n = len(refs) - 2
    zrecvs, (to_prev, to_next) = refs[:n], refs[n:]
    tiles = plan.corner_tiles()
    for k, zrecv in enumerate(zrecvs):
        for t, (i, h, p) in enumerate(tiles):
            t += k * len(tiles)
            to_prev[t] = zrecv[i, h, 8 * p : 8 * p + 8, :]
            low = 4 * plan.Y - plan.hrow + 8 * p
            to_next[t] = zrecv[i, h, low : low + 8, :]


def main_kernel(plan, scal, tables, imp, weights, xv, gown, *refs):
    n = 0 if plan.D == 1 else 1 if plan.swap else 2
    zrecvs, from_prev, from_next = refs[:n], refs[n], refs[n + 1]
    corners = refs[n + 2 : len(refs) - 11]
    out_u, out_v = refs[len(refs) - 11 : len(refs) - 9]
    U, V, DM, lam, mu, G, CI, F, KB = refs[len(refs) - 9 :]
    Z, Y, X, H, T = plan.Z, plan.Y, plan.X, plan.H, plan.T
    PB, P0, R, ZB, ZS, YB = plan.PB, plan.P0, plan.hrow, plan.ZB, plan.ZS, plan.YB
    offset = scal[1]
    halves = range(H)
    row = lax.broadcasted_iota(jnp.int32, (8, LANES), 0)
    lane = lax.broadcasted_iota(jnp.int32, (8, LANES), 1)
    first_half = row < 4
    spare = (row == 3) | (row == 7)
    zero = jnp.zeros((8, LANES), f32)

    def shift_left(parts):
        rolled = [pltpu.roll(p, LANES - 1, 1) for p in parts] + [zero]
        return [jnp.where(lane == LANES - 1, rolled[h + 1], rolled[h]) for h in halves]

    def shift_right(parts):
        rolled = [zero] + [pltpu.roll(p, 1, 1) for p in parts]
        return [jnp.where(lane == 0, rolled[h], rolled[h + 1]) for h in halves]

    def columns(parts):
        ahead = shift_left(parts)
        tiles = []
        for h in halves:
            swapped = pltpu.roll(ahead[h], 4, 0)
            even = jnp.where(first_half, parts[h], swapped)
            odd = jnp.where(first_half, swapped, parts[h])
            high0 = even.astype(bf16).astype(f32)
            high1 = odd.astype(bf16).astype(f32)
            tiles.append(
                (
                    jnp.concatenate([high0, even - high0], 0).astype(bf16),
                    jnp.concatenate([high0, high1], 0).astype(bf16),
                    jnp.concatenate([high1, odd - high1], 0).astype(bf16),
                )
            )
        return tiles

    def put_columns(buffers, z, p, parts):
        for h, tiles in enumerate(columns(parts)):
            for j in range(3):
                for b in buffers:
                    KB[b, z, p, 16 * j : 16 * j + 16, h * LANES : (h + 1) * LANES] = tiles[j]

    mid = slice(R, R + 4 * Y)
    for z in range(Z):
        U[offset + z, :, mid, :] = xv[z, :, : 4 * Y, :]
        V[offset + z, :, mid, :] = xv[z, :, 4 * Y :, :]
    for zrecv, (at_u, at_v, lacks) in zip(zrecvs, halo_places(plan, scal)):
        for i in range(T):
            U[at_u + i, :, mid, :] = zrecv[i]
        for i in range(T - 1):
            V[at_v + i, :, mid, :] = zrecv[T + i]
        V[lacks, :, mid, :] = jnp.zeros((H, 4 * Y, LANES), f32)
    U[ZB:, :, :, :] = jnp.zeros((ZS - ZB, H, 4 * YB, LANES), f32)
    V[ZB:, :, :, :] = jnp.zeros((ZS - ZB, H, 4 * YB, LANES), f32)
    for s in range(T):
        G[s] = jnp.zeros((H, 4 * YB, LANES), f32)
        G[s, :, mid, :] = gown[s]
    own, waves = plan.own_tiles()
    for source, low in ((from_prev, 0), (from_next, R + 4 * Y)):
        for t, (f, z, h, p) in enumerate(own):
            (V if f else U)[offset + z, h, low + 8 * p : low + 8 * p + 8, :] = source[t]
        for t, (s, h, k, n_pairs) in enumerate(waves):
            at = (R - 8 * n_pairs if low == 0 else low) + 8 * k
            G[s, h, at : at + 8, :] = source[len(own) + t]
    tiles = plan.corner_tiles()
    for k, (at_u, at_v, lacks) in enumerate(halo_places(plan, scal)):
        for source, low in zip(corners, (0, R + 4 * Y)):
            for t, (i, h, p) in enumerate(tiles):
                at = slice(low + 8 * p, low + 8 * p + 8)
                if i < T:
                    U[at_u + i, h, at, :] = source[k * len(tiles) + t]
                else:
                    V[at_v + i - T, h, at, :] = source[k * len(tiles) + t]
            V[lacks, :, low : low + R, :] = jnp.zeros((H, R, LANES), f32)

    n_levels = tables.shape[1]

    def prepare(z, carry):
        for h in halves:
            for y in range(0, plan.YL, 8):
                count = min(8, YB - y)
                if count == 8:
                    level = U[z, h, pl.ds(4 * y + 3, 8, stride=4), :]
                    first = y
                else:
                    first = YB - 8
                    level = U[z, h, pl.ds(4 * first + 3, 8, stride=4), :]
                dil = jnp.zeros((8, LANES), f32)
                she = jnp.zeros((8, LANES), f32)
                for k in range(n_levels):
                    here = level == float(k + 1)
                    dil = jnp.where(here, tables[0, k], dil)
                    she = jnp.where(here, tables[1, k], she)
                lam[z, h, first : first + 8, :] = dil
                mu[z, h, first : first + 8, :] = she
        for p in range(PB):
            at = slice(8 * p, 8 * p + 8)
            for h in halves:
                v = V[z, h, at, :]
                mass = jnp.where(
                    first_half,
                    jnp.broadcast_to(v[3:4, :], (8, LANES)),
                    jnp.broadcast_to(v[7:8, :], (8, LANES)),
                )
                DM[z, h, at, :] = jnp.where(spare, 0.0, time_step * mass)
            put_columns((0, 1), z, p, [U[z, h, at, :] for h in halves])
        for b in range(2):
            KB[b, z, PB] = jnp.zeros((48, X), bf16)
        return carry

    lax.fori_loop(0, ZS, prepare, 0)

    bottom = offset + Z - 1
    wave = jnp.zeros((8, LANES), f32)
    for c in range(3):
        wave = jnp.where((row == c) | (row == 4 + c), imp[c], wave)
    wave = jnp.where(scal[2] == 1, wave, zero)
    for h in halves:
        for p in range(PB):
            at = slice(8 * p, 8 * p + 8)
            CI[h, at, :] = wave * DM[bottom, h, at, :]

    def one_step(s, final):
        d = T - 1 - s
        cur, new = s % 2, 1 - s % 2
        p_first = (plan.hy - d - 1) // 2
        p_last = (plan.hy + Y - 1 + d) // 2
        if plan.D == 1:
            p_z0, count = 0, -(-Z // 2)
        elif plan.swap:
            top = scal[0] == 0
            count = -(-(Z + d + 1) // 2)
            p_z0 = jnp.where(top, 0, ZB - 2 * count)
        else:
            p_z0 = T - d - 1
            count = -(-(Z + 2 * d + 1) // 2)

        for p in range(p_first, p_last + 1):
            at = slice(8 * p, 8 * p + 8)
            for h in halves:
                v = V[bottom, h, at, :]
                V[bottom, h, at, :] = v + CI[h, at, :] * (G[s, h, at, :] - v)
        for p in range(p_first, p_last + 1):
            F[p] = jnp.zeros((2, H, 8, LANES), f32)

        def finish(z, p, g0, g1):
            at = slice(8 * p, 8 * p + 8)
            other = [
                pltpu.roll(jnp.where(first_half, g1[h], g0[h]), 4, 0) for h in halves
            ]
            other = shift_right(other)
            fresh = []
            for h in halves:
                force = jnp.where(first_half, g0[h], g1[h]) + other[h]
                v = V[z, h, at, :] - DM[z, h, at, :] * force
                u = U[z, h, at, :] + time_step * v
                V[z, h, at, :] = v
                U[z, h, at, :] = u
                fresh.append(u)
            if not final:
                put_columns((new,), z, p, fresh)

        def two_layers(i, carry):
            z0 = p_z0 + 2 * i
            side = [[zero for _ in halves] for _ in range(3)]
            for p in range(p_first, p_last + 1):
                right = jnp.concatenate(
                    [
                        KB[cur, z0, p],
                        KB[cur, z0, p + 1, :32],
                        KB[cur, z0 + 1, p],
                        KB[cur, z0 + 1, p + 1, :32],
                        KB[cur, z0 + 2, p],
                        KB[cur, z0 + 2, p + 1],
                    ],
                    0,
                )
                product = jnp.dot(weights[...], right, preferred_element_type=f32)
                node = [[None] * 3 for _ in range(3)]
                for zn in range(3):
                    node[zn][0] = side[zn]
                for y in range(2):
                    above = [F[p, y, h] for h in halves]
                    node[0][y] = above if y else [a + b for a, b in zip(node[0][0], above)]
                for ez in range(2):
                    for ey in range(2):
                        base = 64 * (2 * ez + ey)
                        y = 2 * p + ey
                        for h in halves:
                            lanes = slice(h * LANES, (h + 1) * LANES)
                            dil = jnp.broadcast_to(lam[z0 + ez, h, y : y + 1, :], (8, LANES))
                            she = jnp.broadcast_to(mu[z0 + ez, h, y : y + 1, :], (8, LANES))
                            for dz in range(2):
                                for dy in range(2):
                                    r = base + 8 * (2 * dz + dy)
                                    part = (
                                        dil * product[r : r + 8, lanes]
                                        + she * product[r + 32 : r + 40, lanes]
                                    )
                                    slot = node[ez + dz][ey + dy]
                                    if slot is None:
                                        slot = node[ez + dz][ey + dy] = [None] * H
                                    elif slot is side[ez + dz]:
                                        slot = node[ez + dz][ey + dy] = list(slot)
                                    slot[h] = part if slot[h] is None else slot[h] + part
                for y in range(2):
                    for h in halves:
                        F[p, y, h] = node[2][y][h]
                finish(z0, p, node[0][0], node[0][1])
                finish(z0 + 1, p, node[1][0], node[1][1])
                side = [node[zn][2] for zn in range(3)]
            return carry

        def chunk(first, rows):
            for i in range(rows):
                two_layers(first + i, 0)

        U3 = 3
        full, rest = count // U3, count % U3
        if full:
            lax.fori_loop(0, full * scal[3], lambda i, c: (chunk(U3 * i, U3), c)[1], 0)
        if rest:
            lax.fori_loop(0, scal[3], lambda i, c: (chunk(U3 * full, rest), c)[1], 0)

    for s in range(T):
        one_step(s, s == T - 1)

    for z in range(Z):
        for h in halves:
            lanes = slice(h * LANES, (h + 1) * LANES)
            for y in range(0, Y, 8):
                for c in range(3):
                    at = pl.ds(R + 4 * y + c, 8, stride=4)
                    out_u[c, z, y : y + 8, lanes] = U[offset + z, h, at, :]
                    out_v[c, z, y : y + 8, lanes] = V[offset + z, h, at, :]


def smem():
    return pl.BlockSpec(memory_space=pltpu.SMEM)


def vmem():
    return pl.BlockSpec(memory_space=pltpu.VMEM)


def per_device(plan, u, v, m, mat, dilation_table, shear_table, stiffness_pair, impedance, mask, inc):
    Z, Y, X, H, T, D, L = plan.Z, plan.Y, plan.X, plan.H, plan.T, plan.D, plan.L
    depth = lax.axis_index("depth")
    scal = jnp.stack(
        [depth, jnp.asarray(plan.offset(depth)), (depth == D - 1).astype(jnp.int32), jnp.asarray(1)]
    ).astype(jnp.int32)
    shape = lambda *dims: jax.ShapeDtypeStruct(dims, f32)

    rows, cols = selectors()
    weights = pl.pallas_call(
        matrix_kernel,
        out_shape=jax.ShapeDtypeStruct((256, 256), bf16),
        name="matrix",
    )(stiffness_pair.reshape(48, 24), jnp.asarray(rows, bf16), jnp.asarray(cols, bf16))

    n_sends = 0 if D == 1 else 1 if plan.swap else 2
    tiles, waves = plan.own_tiles()
    edge = shape(len(tiles) + len(waves), 8, LANES)
    packed = pl.pallas_call(
        lambda *refs: pack_kernel(plan, *refs),
        out_shape=[shape(Z, H, 8 * Y, LANES), shape(T, H, 4 * Y, LANES), edge, edge]
        + [shape(2 * T - 1, H, 4 * Y, LANES)] * n_sends,
        in_specs=[smem()] + [vmem()] * 6,
        out_specs=[vmem()] * (4 + n_sends),
        name="pack",
    )(scal, u, v, m, mat, mask, inc)
    xv, g, to_prev, to_next = packed[:4]
    sends = packed[4:]
    up = [(i + 1, i) for i in range(L - 1)]
    down = [(i, i + 1) for i in range(L - 1)]
    if D == 1:
        zrecvs = []
    elif plan.swap:
        zrecvs = [lax.ppermute(sends[0], "depth", [(0, 1), (1, 0)])]
    else:
        zrecvs = [
            lax.ppermute(sends[0], "depth", [(i, i + 1) for i in range(D - 1)]),
            lax.ppermute(sends[1], "depth", [(i + 1, i) for i in range(D - 1)]),
        ]
    from_next = lax.ppermute(to_prev, "lat", up)
    from_prev = lax.ppermute(to_next, "lat", down)
    corners = []
    if zrecvs:
        corner = shape(len(zrecvs) * len(plan.corner_tiles()), 8, LANES)
        corner_prev, corner_next = pl.pallas_call(
            lambda *refs: corner_kernel(plan, *refs),
            out_shape=[corner, corner],
            in_specs=[vmem()] * len(zrecvs),
            out_specs=[vmem()] * 2,
            name="corner",
        )(*zrecvs)
        corners = [lax.ppermute(corner_next, "lat", down), lax.ppermute(corner_prev, "lat", up)]
    tables = jnp.stack([dilation_table, shear_table])
    grid = (plan.ZS, H, 4 * plan.YB, LANES)
    new_u, new_v = pl.pallas_call(
        lambda *refs: main_kernel(plan, *refs),
        out_shape=[shape(3, Z, Y, X)] * 2,
        in_specs=[smem()] * 3 + [vmem()] * (5 + len(zrecvs) + len(corners)),
        out_specs=[vmem()] * 2,
        scratch_shapes=[
            pltpu.VMEM(grid, f32),
            pltpu.VMEM(grid, f32),
            pltpu.VMEM(grid, f32),
            pltpu.VMEM((plan.ZS, H, plan.YL, LANES), f32),
            pltpu.VMEM((plan.ZS, H, plan.YL, LANES), f32),
            pltpu.VMEM((T, H, 4 * plan.YB, LANES), f32),
            pltpu.VMEM((H, 4 * plan.YB, LANES), f32),
            pltpu.VMEM((plan.PB, 2, H, 8, LANES), f32),
            pltpu.VMEM((2, plan.ZS, plan.PB + 1, 48, X), bf16),
        ],
        name="steps",
    )(scal, tables, impedance, weights, xv, g, *zrecvs, from_prev, from_next, *corners)
    return new_u, new_v


def solution(mesh):
    field = P(None, "depth", "lat", None)
    in_specs = (
        field,
        field,
        P("depth", "lat", None),
        P("depth", "lat", None),
        P(),
        P(),
        P(),
        P(),
        P("lat", None),
        P(None, None, "lat", None),
    )

    def whole(displacement, *rest):
        plan = Plan(mesh, displacement, rest[-1])
        return jax.shard_map(
            lambda *args: per_device(plan, *args),
            mesh=mesh,
            in_specs=in_specs,
            out_specs=(field, field),
            check_vma=False,
        )(displacement, *rest)

    return whole
```

```python
import jax
import jax.numpy as jnp
import numpy as np
from jax import lax
from jax.experimental import pallas as pl
from jax.experimental.pallas import tpu as pltpu
from jax.sharding import PartitionSpec as P

time_step = 0.1
LANES = 128
f32 = jnp.float32
bf16 = jnp.bfloat16


class Plan:
    def __init__(self, mesh, displacement, incident):
        self.D = mesh.shape["depth"]
        self.L = mesh.shape["lat"]
        self.Z = displacement.shape[1] // self.D
        self.Y = displacement.shape[2] // self.L
        self.X = displacement.shape[3]
        self.H = self.X // LANES
        self.T = incident.shape[0]
        T = self.T
        assert T <= self.Z and T <= self.Y and self.Y % 8 == 0
        assert self.X % LANES == 0
        self.hy = T + T % 2
        self.YB = self.Y + 2 * self.hy
        self.PB = self.YB // 2
        self.P0 = self.hy // 2
        self.swap = self.D == 2
        self.ZB = self.Z + (0 if self.D == 1 else T if self.swap else 2 * T)
        self.ZS = self.ZB + 2
        self.YL = -(-self.YB // 8) * 8
        self.gpairs = [-(-(T - 1 - s) // 2) for s in range(T)]
        self.hrow = 4 * self.hy

    def offset(self, depth):
        if self.D == 1:
            return 0
        return depth * self.T if self.swap else self.T

    def own_tiles(self):
        n = self.hy // 2
        tiles = [(f, z, h, p) for f in (0, 1) for z in range(self.Z) for h in range(self.H) for p in range(n)]
        waves = [
            (s, h, k, n_pairs)
            for s, n_pairs in enumerate(self.gpairs)
            for h in range(self.H)
            for k in range(n_pairs)
        ]
        return tiles, waves

    def corner_tiles(self):
        n = self.hy // 2
        return [(i, h, p) for i in range(2 * self.T - 1) for h in range(self.H) for p in range(n)]


def selectors():
    rows = np.zeros((4, 64, 48), np.float32)
    cols = np.zeros((2, 4, 24, 256), np.float32)

    def half(parity, dx):
        return 4 * (dx ^ parity)

    blocks = [(0, 0, 0), (8, 0, 0), (16, 0, 1), (24, 1, 1), (32, 1, 0), (40, 1, 0), (48, 2, 0), (56, 2, 0), (64, 2, 1)]
    for ez in range(2):
        for ey in range(2):
            e = 2 * ez + ey
            for lm in range(2):
                for dz in range(2):
                    for dy in range(2):
                        for dx in range(2):
                            for c in range(3):
                                dof = (4 * dz + 2 * dy + dx) * 3 + c
                                r = half((ey + dy) % 2, dx) + c
                                rows[e, ((lm * 2 + dz) * 2 + dy) * 8 + r, lm * 24 + dof] = 1
            for base, node, low in blocks:
                for zn in range(3):
                    dz, dy = zn - ez, node - ey
                    if dz in (0, 1) and dy in (0, 1):
                        for dx in range(2):
                            for c in range(3):
                                dof = (4 * dz + 2 * dy + dx) * 3 + c
                                cols[low, e, dof, zn * 80 + base + half(node % 2, dx) + c] = 1
    return rows, cols


def matrix_kernel(stiff_ref, rows_ref, cols_ref, out_ref):
    stiff = stiff_ref[...]
    high = stiff.astype(bf16)
    low = (stiff - high.astype(f32)).astype(bf16)
    for e in range(4):
        total = None
        for part, k in ((high, 0), (low, 1)):
            picked = jnp.dot(rows_ref[e], part, preferred_element_type=f32).astype(bf16)
            placed = jnp.dot(picked, cols_ref[k, e], preferred_element_type=f32)
            total = placed if total is None else total + placed
        out_ref[64 * e : 64 * e + 64, :] = total.astype(bf16)


def pack_kernel(plan, u, v, m, mat, mask, inc, xv, g, to_prev, to_next, *zsends):
    Z, Y, H, T = plan.Z, plan.Y, plan.H, plan.T
    scal = place(plan)
    for z in range(Z):
        for h in range(H):
            lanes = slice(h * LANES, (h + 1) * LANES)
            for y in range(0, Y, 8):
                rows = slice(y, y + 8)
                for c in range(3):
                    xv[z, h, pl.ds(4 * y + c, 8, stride=4), :] = u[c, z, rows, lanes]
                    xv[z, h, pl.ds(4 * (Y + y) + c, 8, stride=4), :] = v[c, z, rows, lanes]
                xv[z, h, pl.ds(4 * y + 3, 8, stride=4), :] = mat[z, rows, lanes].astype(f32) + 1.0
                xv[z, h, pl.ds(4 * (Y + y) + 3, 8, stride=4), :] = m[z, rows, lanes]
    for h in range(H):
        lanes = slice(h * LANES, (h + 1) * LANES)
        for y in range(0, Y, 8):
            rows = slice(y, y + 8)
            double = 2.0 * mask[rows, lanes].astype(f32)
            for s in range(T):
                for c in range(3):
                    g[s, h, pl.ds(4 * y + c, 8, stride=4), :] = double * inc[s, c, rows, lanes]
                g[s, h, pl.ds(4 * y + 3, 8, stride=4), :] = jnp.zeros((8, LANES), f32)
    tiles, waves = plan.own_tiles()
    for out, low in ((to_prev, 0), (to_next, 4 * Y - plan.hrow)):
        for t, (f, z, h, p) in enumerate(tiles):
            at = 4 * Y * f + low + 8 * p
            out[t] = xv[z, h, at : at + 8, :]
        for t, (s, h, k, n_pairs) in enumerate(waves):
            at = 8 * k if low == 0 else 4 * Y - 8 * n_pairs + 8 * k
            out[len(tiles) + t] = g[s, h, at : at + 8, :]
    for k, zsend in enumerate(zsends):
        if plan.swap:
            first = jnp.where(scal[0] == 0, Z - T, 0)
            first_v = jnp.where(scal[0] == 0, Z - T + 1, 0)
        else:
            first, first_v = (Z - T, Z - T + 1) if k == 0 else (0, 0)
        for i in range(T):
            zsend[i] = xv[first + i, :, : 4 * Y, :]
        for i in range(T - 1):
            zsend[T + i] = xv[first_v + i, :, 4 * Y :, :]


def place(plan):
    depth = lax.axis_index("depth")
    one = (depth >= 0).astype(jnp.int32)
    return depth, plan.offset(depth), (depth == plan.D - 1).astype(jnp.int32), one


def halo_places(plan, scal):
    if plan.D == 1:
        return []
    if plan.swap:
        top = scal[0] == 0
        return [
            (
                jnp.where(top, plan.Z, 0),
                jnp.where(top, plan.Z, 1),
                jnp.where(top, plan.Z + plan.T - 1, 0),
            )
        ]
    last = plan.T + plan.Z
    return [(0, 1, 0), (last, last, last + plan.T - 1)]


def corner_kernel(plan, *refs):
    n = len(refs) - 2
    zrecvs, (to_prev, to_next) = refs[:n], refs[n:]
    tiles = plan.corner_tiles()
    for k, zrecv in enumerate(zrecvs):
        for t, (i, h, p) in enumerate(tiles):
            t += k * len(tiles)
            to_prev[t] = zrecv[i, h, 8 * p : 8 * p + 8, :]
            low = 4 * plan.Y - plan.hrow + 8 * p
            to_next[t] = zrecv[i, h, low : low + 8, :]


def main_kernel(plan, dilations, shears, imp, weights, xv, gown, *refs):
    n = 0 if plan.D == 1 else 1 if plan.swap else 2
    zrecvs, from_prev, from_next = refs[:n], refs[n], refs[n + 1]
    corners = refs[n + 2 : len(refs) - 11]
    out_u, out_v = refs[len(refs) - 11 : len(refs) - 9]
    U, V, DM, lam, mu, G, CI, F, KB = refs[len(refs) - 9 :]
    Z, Y, X, H, T = plan.Z, plan.Y, plan.X, plan.H, plan.T
    PB, P0, R, ZB, ZS, YB = plan.PB, plan.P0, plan.hrow, plan.ZB, plan.ZS, plan.YB
    scal = place(plan)
    offset = scal[1]
    halves = range(H)
    row = lax.broadcasted_iota(jnp.int32, (8, LANES), 0)
    lane = lax.broadcasted_iota(jnp.int32, (8, LANES), 1)
    first_half = row < 4
    spare = (row == 3) | (row == 7)
    zero = jnp.zeros((8, LANES), f32)

    def shift_left(parts):
        rolled = [pltpu.roll(p, LANES - 1, 1) for p in parts] + [zero]
        return [jnp.where(lane == LANES - 1, rolled[h + 1], rolled[h]) for h in halves]

    def shift_right(parts):
        rolled = [zero] + [pltpu.roll(p, 1, 1) for p in parts]
        return [jnp.where(lane == 0, rolled[h], rolled[h + 1]) for h in halves]

    def columns(parts):
        ahead = shift_left(parts)
        tiles = []
        for h in halves:
            swapped = pltpu.roll(ahead[h], 4, 0)
            even = jnp.where(first_half, parts[h], swapped)
            odd = jnp.where(first_half, swapped, parts[h])
            high0 = even.astype(bf16).astype(f32)
            high1 = odd.astype(bf16).astype(f32)
            tiles.append(
                (
                    jnp.concatenate([high0, even - high0], 0).astype(bf16),
                    jnp.concatenate([high0, high1], 0).astype(bf16),
                    jnp.concatenate([high1, odd - high1], 0).astype(bf16),
                )
            )
        return tiles

    def put_columns(buffers, z, p, parts):
        for h, tiles in enumerate(columns(parts)):
            for j in range(3):
                for b in buffers:
                    KB[b, z, p, 16 * j : 16 * j + 16, h * LANES : (h + 1) * LANES] = tiles[j]

    mid = slice(R, R + 4 * Y)
    for z in range(Z):
        U[offset + z, :, mid, :] = xv[z, :, : 4 * Y, :]
        V[offset + z, :, mid, :] = xv[z, :, 4 * Y :, :]
    for zrecv, (at_u, at_v, lacks) in zip(zrecvs, halo_places(plan, scal)):
        for i in range(T):
            U[at_u + i, :, mid, :] = zrecv[i]
        for i in range(T - 1):
            V[at_v + i, :, mid, :] = zrecv[T + i]
        V[lacks, :, mid, :] = jnp.zeros((H, 4 * Y, LANES), f32)
    U[ZB:, :, :, :] = jnp.zeros((ZS - ZB, H, 4 * YB, LANES), f32)
    V[ZB:, :, :, :] = jnp.zeros((ZS - ZB, H, 4 * YB, LANES), f32)
    for s in range(T):
        G[s] = jnp.zeros((H, 4 * YB, LANES), f32)
        G[s, :, mid, :] = gown[s]
    own, waves = plan.own_tiles()
    for source, low in ((from_prev, 0), (from_next, R + 4 * Y)):
        for t, (f, z, h, p) in enumerate(own):
            (V if f else U)[offset + z, h, low + 8 * p : low + 8 * p + 8, :] = source[t]
        for t, (s, h, k, n_pairs) in enumerate(waves):
            at = (R - 8 * n_pairs if low == 0 else low) + 8 * k
            G[s, h, at : at + 8, :] = source[len(own) + t]
    tiles = plan.corner_tiles()
    for k, (at_u, at_v, lacks) in enumerate(halo_places(plan, scal)):
        for source, low in zip(corners, (0, R + 4 * Y)):
            for t, (i, h, p) in enumerate(tiles):
                at = slice(low + 8 * p, low + 8 * p + 8)
                if i < T:
                    U[at_u + i, h, at, :] = source[k * len(tiles) + t]
                else:
                    V[at_v + i - T, h, at, :] = source[k * len(tiles) + t]
            V[lacks, :, low : low + R, :] = jnp.zeros((H, R, LANES), f32)

    n_levels = dilations.shape[0]

    def prepare(z, carry):
        for h in halves:
            for y in range(0, plan.YL, 8):
                count = min(8, YB - y)
                if count == 8:
                    level = U[z, h, pl.ds(4 * y + 3, 8, stride=4), :]
                    first = y
                else:
                    first = YB - 8
                    level = U[z, h, pl.ds(4 * first + 3, 8, stride=4), :]
                dil = jnp.zeros((8, LANES), f32)
                she = jnp.zeros((8, LANES), f32)
                for k in range(n_levels):
                    here = level == float(k + 1)
                    dil = jnp.where(here, dilations[k], dil)
                    she = jnp.where(here, shears[k], she)
                lam[z, h, first : first + 8, :] = dil
                mu[z, h, first : first + 8, :] = she
        for p in range(PB):
            at = slice(8 * p, 8 * p + 8)
            for h in halves:
                v = V[z, h, at, :]
                mass = jnp.where(
                    first_half,
                    jnp.broadcast_to(v[3:4, :], (8, LANES)),
                    jnp.broadcast_to(v[7:8, :], (8, LANES)),
                )
                DM[z, h, at, :] = jnp.where(spare, 0.0, time_step * mass)
            put_columns((0, 1), z, p, [U[z, h, at, :] for h in halves])
        for b in range(2):
            KB[b, z, PB] = jnp.zeros((48, X), bf16)
        return carry

    lax.fori_loop(0, ZS, prepare, 0)

    bottom = offset + Z - 1
    wave = jnp.zeros((8, LANES), f32)
    for c in range(3):
        wave = jnp.where((row == c) | (row == 4 + c), imp[c], wave)
    wave = jnp.where(scal[2] == 1, wave, zero)
    for h in halves:
        for p in range(PB):
            at = slice(8 * p, 8 * p + 8)
            CI[h, at, :] = wave * DM[bottom, h, at, :]

    def one_step(s, final):
        d = T - 1 - s
        cur, new = s % 2, 1 - s % 2
        p_first = (plan.hy - d - 1) // 2
        p_last = (plan.hy + Y - 1 + d) // 2
        if plan.D == 1:
            p_z0, count = 0, -(-Z // 2)
        elif plan.swap:
            top = scal[0] == 0
            count = -(-(Z + d + 1) // 2)
            p_z0 = jnp.where(top, 0, ZB - 2 * count)
        else:
            p_z0 = T - d - 1
            count = -(-(Z + 2 * d + 1) // 2)

        for p in range(p_first, p_last + 1):
            at = slice(8 * p, 8 * p + 8)
            for h in halves:
                v = V[bottom, h, at, :]
                V[bottom, h, at, :] = v + CI[h, at, :] * (G[s, h, at, :] - v)
        for p in range(p_first, p_last + 1):
            F[p] = jnp.zeros((2, H, 8, LANES), f32)

        def finish(z, p, g0, g1):
            at = slice(8 * p, 8 * p + 8)
            other = [
                pltpu.roll(jnp.where(first_half, g1[h], g0[h]), 4, 0) for h in halves
            ]
            other = shift_right(other)
            fresh = []
            for h in halves:
                force = jnp.where(first_half, g0[h], g1[h]) + other[h]
                v = V[z, h, at, :] - DM[z, h, at, :] * force
                u = U[z, h, at, :] + time_step * v
                V[z, h, at, :] = v
                U[z, h, at, :] = u
                fresh.append(u)
            if not final:
                put_columns((new,), z, p, fresh)

        def two_layers(i, carry):
            z0 = p_z0 + 2 * i
            side = [[zero for _ in halves] for _ in range(3)]
            for p in range(p_first, p_last + 1):
                right = jnp.concatenate(
                    [
                        KB[cur, z0, p],
                        KB[cur, z0, p + 1, :32],
                        KB[cur, z0 + 1, p],
                        KB[cur, z0 + 1, p + 1, :32],
                        KB[cur, z0 + 2, p],
                        KB[cur, z0 + 2, p + 1],
                    ],
                    0,
                )
                product = jnp.dot(weights[...], right, preferred_element_type=f32)
                node = [[None] * 3 for _ in range(3)]
                for zn in range(3):
                    node[zn][0] = side[zn]
                for y in range(2):
                    above = [F[p, y, h] for h in halves]
                    node[0][y] = above if y else [a + b for a, b in zip(node[0][0], above)]
                for ez in range(2):
                    for ey in range(2):
                        base = 64 * (2 * ez + ey)
                        y = 2 * p + ey
                        for h in halves:
                            lanes = slice(h * LANES, (h + 1) * LANES)
                            dil = jnp.broadcast_to(lam[z0 + ez, h, y : y + 1, :], (8, LANES))
                            she = jnp.broadcast_to(mu[z0 + ez, h, y : y + 1, :], (8, LANES))
                            for dz in range(2):
                                for dy in range(2):
                                    r = base + 8 * (2 * dz + dy)
                                    part = (
                                        dil * product[r : r + 8, lanes]
                                        + she * product[r + 32 : r + 40, lanes]
                                    )
                                    slot = node[ez + dz][ey + dy]
                                    if slot is None:
                                        slot = node[ez + dz][ey + dy] = [None] * H
                                    elif slot is side[ez + dz]:
                                        slot = node[ez + dz][ey + dy] = list(slot)
                                    slot[h] = part if slot[h] is None else slot[h] + part
                for y in range(2):
                    for h in halves:
                        F[p, y, h] = node[2][y][h]
                finish(z0, p, node[0][0], node[0][1])
                finish(z0 + 1, p, node[1][0], node[1][1])
                side = [node[zn][2] for zn in range(3)]
            return carry

        def chunk(first, rows):
            for i in range(rows):
                two_layers(first + i, 0)

        straight = count if plan.ZB <= 16 else 1
        full, rest = count // straight, count % straight
        lax.fori_loop(0, full * scal[3], lambda i, c: (chunk(straight * i, straight), c)[1], 0)
        assert rest == 0

    for s in range(T):
        one_step(s, s == T - 1)

    for z in range(Z):
        for h in halves:
            lanes = slice(h * LANES, (h + 1) * LANES)
            for y in range(0, Y, 8):
                for c in range(3):
                    at = pl.ds(R + 4 * y + c, 8, stride=4)
                    out_u[c, z, y : y + 8, lanes] = U[offset + z, h, at, :]
                    out_v[c, z, y : y + 8, lanes] = V[offset + z, h, at, :]


def smem():
    return pl.BlockSpec(memory_space=pltpu.SMEM)


def vmem():
    return pl.BlockSpec(memory_space=pltpu.VMEM)


def per_device(plan, u, v, m, mat, dilation_table, shear_table, stiffness_pair, impedance, mask, inc):
    Z, Y, X, H, T, D, L = plan.Z, plan.Y, plan.X, plan.H, plan.T, plan.D, plan.L
    shape = lambda *dims: jax.ShapeDtypeStruct(dims, f32)

    room = pltpu.CompilerParams(vmem_limit_bytes=40 * 2**20)
    rows, cols = selectors()
    weights = pl.pallas_call(
        matrix_kernel,
        out_shape=pltpu.VMEM((256, 256), bf16),
        compiler_params=room,
        name="matrix",
    )(stiffness_pair.reshape(48, 24), jnp.asarray(rows, bf16), jnp.asarray(cols, bf16))

    n_sends = 0 if D == 1 else 1 if plan.swap else 2
    tiles, waves = plan.own_tiles()
    local = lambda *dims: pltpu.VMEM(dims, f32)
    edge = local(len(tiles) + len(waves), 8, LANES)
    packed = pl.pallas_call(
        lambda *refs: pack_kernel(plan, *refs),
        out_shape=[local(Z, H, 8 * Y, LANES), local(T, H, 4 * Y, LANES), edge, edge]
        + [local(2 * T - 1, H, 4 * Y, LANES)] * n_sends,
        in_specs=[vmem()] * 6,
        out_specs=[vmem()] * (4 + n_sends),
        compiler_params=room,
        name="pack",
    )(*[pltpu.with_memory_space_constraint(a, pltpu.HBM) for a in (u, v, m, mat, mask, inc)])
    xv, g, to_prev, to_next = packed[:4]
    sends = packed[4:]
    up = [(i + 1, i) for i in range(L - 1)]
    down = [(i, i + 1) for i in range(L - 1)]
    if D == 1:
        zrecvs = []
    elif plan.swap:
        zrecvs = [lax.ppermute(sends[0], "depth", [(0, 1), (1, 0)])]
    else:
        zrecvs = [
            lax.ppermute(sends[0], "depth", [(i, i + 1) for i in range(D - 1)]),
            lax.ppermute(sends[1], "depth", [(i + 1, i) for i in range(D - 1)]),
        ]
    from_next = lax.ppermute(to_prev, "lat", up)
    from_prev = lax.ppermute(to_next, "lat", down)
    corners = []
    if zrecvs:
        corner = local(len(zrecvs) * len(plan.corner_tiles()), 8, LANES)
        corner_prev, corner_next = pl.pallas_call(
            lambda *refs: corner_kernel(plan, *refs),
            out_shape=[corner, corner],
            in_specs=[vmem()] * len(zrecvs),
            out_specs=[vmem()] * 2,
            compiler_params=room,
            name="corner",
        )(*[pltpu.with_memory_space_constraint(a, pltpu.VMEM) for a in zrecvs])
        corners = [lax.ppermute(corner_next, "lat", down), lax.ppermute(corner_prev, "lat", up)]
    near = lambda arrays: [pltpu.with_memory_space_constraint(a, pltpu.VMEM) for a in arrays]
    zrecvs, corners = near(zrecvs), near(corners)
    from_prev, from_next, xv, g, weights = near([from_prev, from_next, xv, g, weights])
    grid = (plan.ZS, H, 4 * plan.YB, LANES)
    new_u, new_v = pl.pallas_call(
        lambda *refs: main_kernel(plan, *refs),
        out_shape=[shape(3, Z, Y, X)] * 2,
        in_specs=[smem()] * 3 + [vmem()] * (5 + len(zrecvs) + len(corners)),
        out_specs=[vmem()] * 2,
        scratch_shapes=[
            pltpu.VMEM(grid, f32),
            pltpu.VMEM(grid, f32),
            pltpu.VMEM(grid, f32),
            pltpu.VMEM((plan.ZS, H, plan.YL, LANES), f32),
            pltpu.VMEM((plan.ZS, H, plan.YL, LANES), f32),
            pltpu.VMEM((T, H, 4 * plan.YB, LANES), f32),
            pltpu.VMEM((H, 4 * plan.YB, LANES), f32),
            pltpu.VMEM((plan.PB, 2, H, 8, LANES), f32),
            pltpu.VMEM((2, plan.ZS, plan.PB + 1, 48, X), bf16),
        ],
        compiler_params=room,
        name="steps",
    )(dilation_table, shear_table, impedance, weights, xv, g, *zrecvs, from_prev, from_next, *corners)
    return new_u, new_v


def solution(mesh):
    field = P(None, "depth", "lat", None)
    in_specs = (
        field,
        field,
        P("depth", "lat", None),
        P("depth", "lat", None),
        P(),
        P(),
        P(),
        P(),
        P("lat", None),
        P(None, None, "lat", None),
    )

    def whole(displacement, *rest):
        plan = Plan(mesh, displacement, rest[-1])
        return jax.shard_map(
            lambda *args: per_device(plan, *args),
            mesh=mesh,
            in_specs=in_specs,
            out_specs=(field, field),
            check_vma=False,
        )(displacement, *rest)

    return whole
```

```python
import jax
import jax.numpy as jnp
import numpy as np
from jax import lax
from jax.experimental import pallas as pl
from jax.experimental.pallas import tpu as pltpu
from jax.sharding import PartitionSpec as P

time_step = 0.1
LANES = 128
f32 = jnp.float32
bf16 = jnp.bfloat16


class Plan:
    def __init__(self, mesh, displacement, incident):
        self.D = mesh.shape["depth"]
        self.L = mesh.shape["lat"]
        self.Z = displacement.shape[1] // self.D
        self.Y = displacement.shape[2] // self.L
        self.X = displacement.shape[3]
        self.H = self.X // LANES
        self.T = incident.shape[0]
        T = self.T
        assert T <= self.Z and T <= self.Y and self.Y % 8 == 0
        assert self.X % LANES == 0
        self.hy = T + T % 2
        self.YB = self.Y + 2 * self.hy
        self.PB = self.YB // 2
        self.P0 = self.hy // 2
        self.swap = self.D == 2
        self.ZB = self.Z + (0 if self.D == 1 else T if self.swap else 2 * T)
        self.ZS = self.ZB + 2
        self.YL = -(-self.YB // 8) * 8
        self.gpairs = [-(-(T - 1 - s) // 2) for s in range(T)]
        self.hrow = 4 * self.hy

    def offset(self, depth):
        if self.D == 1:
            return 0
        return depth * self.T if self.swap else self.T

    def halo_tiles(self, u_layers, v_layers):
        n = self.hy // 2
        tiles = [("u", z, h, p) for z in u_layers for h in range(self.H) for p in range(n)]
        tiles += [("v", z, h, p) for z in v_layers for h in range(self.H) for p in range(n - 1)]
        if self.T % 2 == 0:
            tiles += [("half", z, h, 0) for z in v_layers for h in range(0, self.H, 2)]
        return tiles

    def own_tiles(self):
        return self.halo_tiles(range(self.Z), range(self.Z)), [
            (s, h, k, n_pairs)
            for s, n_pairs in enumerate(self.gpairs)
            for h in range(self.H)
            for k in range(n_pairs)
        ]

    def corner_tiles(self):
        return self.halo_tiles(range(self.T), range(self.T, 2 * self.T - 1))

    def sides(self):
        odd = lax.rem(lax.axis_index("lat"), jnp.int32(2))
        return odd == 1, odd == 0


def aligned(value):
    return pl.multiple_of(value, 8)


def first_half():
    return lax.broadcasted_iota(jnp.int32, (8, LANES), 0) < 4


def put_halo(plan, tiles, out, start, to_next, read):
    n, R, top = plan.hy // 2, plan.hrow, 4 * plan.Y - plan.hrow
    u_low = jnp.where(to_next, top, 0)
    v_low = jnp.where(to_next, top + 8, 0)
    far = jnp.where(to_next, top, R - 8)
    for t, (kind, z, h, p) in enumerate(tiles):
        if kind == "half":
            a, b = read("v", z, h, aligned(far)), read("v", z, h + 1, aligned(far))
            low = jnp.where(first_half(), a, pltpu.roll(b, 4, 0))
            high = jnp.where(first_half(), pltpu.roll(a, 4, 0), b)
            out[start + t] = jnp.where(to_next, high, low)
        else:
            out[start + t] = read(kind, z, h, aligned((u_low if kind == "u" else v_low) + 8 * p))


def take_halo(plan, tiles, source, start, from_next, write):
    n, R = plan.hy // 2, plan.hrow
    u_low = jnp.where(from_next, R + 4 * plan.Y, 0)
    v_low = jnp.where(from_next, R + 4 * plan.Y, 8)
    far = jnp.where(from_next, R + 4 * plan.Y + 8 * (n - 1), 0)
    for t, (kind, z, h, p) in enumerate(tiles):
        tile = source[start + t]
        if kind == "half":
            turned = pltpu.roll(tile, 4, 0)
            keep = first_half() == from_next
            write("v", z, h, aligned(far), jnp.where(keep, jnp.where(from_next, tile, turned), 0.0))
            write("v", z, h + 1, aligned(far), jnp.where(keep, jnp.where(from_next, turned, tile), 0.0))
        else:
            write(kind, z, h, aligned((u_low if kind == "u" else v_low) + 8 * p), tile)


def selectors():
    rows = np.zeros((4, 64, 48), np.float32)
    cols = np.zeros((2, 4, 24, 256), np.float32)

    def half(parity, dx):
        return 4 * (dx ^ parity)

    blocks = [(0, 0, 0), (8, 0, 0), (16, 0, 1), (24, 1, 1), (32, 1, 0), (40, 1, 0), (48, 2, 0), (56, 2, 0), (64, 2, 1)]
    for ez in range(2):
        for ey in range(2):
            e = 2 * ez + ey
            for lm in range(2):
                for dz in range(2):
                    for dy in range(2):
                        for dx in range(2):
                            for c in range(3):
                                dof = (4 * dz + 2 * dy + dx) * 3 + c
                                r = half((ey + dy) % 2, dx) + c
                                rows[e, ((lm * 2 + dz) * 2 + dy) * 8 + r, lm * 24 + dof] = 1
            for base, node, low in blocks:
                for zn in range(3):
                    dz, dy = zn - ez, node - ey
                    if dz in (0, 1) and dy in (0, 1):
                        for dx in range(2):
                            for c in range(3):
                                dof = (4 * dz + 2 * dy + dx) * 3 + c
                                cols[low, e, dof, zn * 80 + base + half(node % 2, dx) + c] = 1
    return rows, cols


def matrix_kernel(stiff_ref, rows_ref, cols_ref, dilations, shears, imp, out_ref, tiles_ref):
    stiff = stiff_ref[...]
    high = stiff.astype(bf16)
    low = (stiff - high.astype(f32)).astype(bf16)
    for e in range(4):
        total = None
        for part, k in ((high, 0), (low, 1)):
            picked = jnp.dot(rows_ref[e], part, preferred_element_type=f32).astype(bf16)
            placed = jnp.dot(picked, cols_ref[k, e], preferred_element_type=f32)
            total = placed if total is None else total + placed
        out_ref[64 * e : 64 * e + 64, :] = total.astype(bf16)
    n = dilations.shape[0]
    for k in range(n):
        tiles_ref[k] = jnp.full((8, LANES), dilations[k], f32)
        tiles_ref[n + k] = jnp.full((8, LANES), shears[k], f32)
    row = lax.broadcasted_iota(jnp.int32, (8, LANES), 0)
    wave = jnp.zeros((8, LANES), f32)
    for c in range(3):
        wave = jnp.where((row == c) | (row == 4 + c), imp[c], wave)
    tiles_ref[2 * n] = wave


def pack_kernel(plan, u, v, m, mat, mask, inc, xv, g, to_first, to_second, *zsends):
    Z, Y, H, T = plan.Z, plan.Y, plan.H, plan.T
    scal = place(plan)
    for z in range(Z):
        for h in range(H):
            lanes = slice(h * LANES, (h + 1) * LANES)
            for y in range(0, Y, 8):
                rows = slice(y, y + 8)
                for c in range(3):
                    xv[z, h, pl.ds(4 * y + c, 8, stride=4), :] = u[c, z, rows, lanes]
                    xv[z, h, pl.ds(4 * (Y + y) + c, 8, stride=4), :] = v[c, z, rows, lanes]
                xv[z, h, pl.ds(4 * y + 3, 8, stride=4), :] = mat[z, rows, lanes].astype(f32) + 1.0
                xv[z, h, pl.ds(4 * (Y + y) + 3, 8, stride=4), :] = m[z, rows, lanes]
    for h in range(H):
        lanes = slice(h * LANES, (h + 1) * LANES)
        for y in range(0, Y, 8):
            rows = slice(y, y + 8)
            double = 2.0 * mask[rows, lanes].astype(f32)
            for s in range(T):
                for c in range(3):
                    g[s, h, pl.ds(4 * y + c, 8, stride=4), :] = double * inc[s, c, rows, lanes]
                g[s, h, pl.ds(4 * y + 3, 8, stride=4), :] = jnp.zeros((8, LANES), f32)
    tiles, waves = plan.own_tiles()

    def read(kind, z, h, row):
        return xv[z, h, pl.ds(row + (4 * Y if kind == "v" else 0), 8), :]

    for out, to_next in zip((to_first, to_second), plan.sides()):
        put_halo(plan, tiles, out, 0, to_next, read)
        for t, (s, h, k, n_pairs) in enumerate(waves):
            at = aligned(jnp.where(to_next, 4 * Y - 8 * n_pairs, 0) + 8 * k)
            out[len(tiles) + t] = g[s, h, pl.ds(at, 8), :]
    for k, zsend in enumerate(zsends):
        if plan.swap:
            first = jnp.where(scal[0] == 0, Z - T, 0)
            first_v = jnp.where(scal[0] == 0, Z - T + 1, 0)
        else:
            first, first_v = (Z - T, Z - T + 1) if k == 0 else (0, 0)
        for i in range(T):
            zsend[i] = xv[first + i, :, : 4 * Y, :]
        for i in range(T - 1):
            zsend[T + i] = xv[first_v + i, :, 4 * Y :, :]


def place(plan):
    depth = lax.axis_index("depth")
    one = (depth >= 0).astype(jnp.int32)
    return depth, plan.offset(depth), (depth == plan.D - 1).astype(jnp.int32), one


def halo_places(plan, scal):
    if plan.D == 1:
        return []
    if plan.swap:
        top = scal[0] == 0
        return [
            (
                jnp.where(top, plan.Z, 0),
                jnp.where(top, plan.Z, 1),
                jnp.where(top, plan.Z + plan.T - 1, 0),
            )
        ]
    last = plan.T + plan.Z
    return [(0, 1, 0), (last, last, last + plan.T - 1)]


def corner_kernel(plan, *refs):
    n = len(refs) - 2
    zrecvs, outs = refs[:n], refs[n:]
    tiles = plan.corner_tiles()
    for out, to_next in zip(outs, plan.sides()):
        for k, zrecv in enumerate(zrecvs):

            def read(kind, i, h, row):
                return zrecv[i, h, pl.ds(row, 8), :]

            put_halo(plan, tiles, out, k * len(tiles), to_next, read)


def main_kernel(plan, tables, weights, xv, gown, *refs):
    n = 0 if plan.D == 1 else 1 if plan.swap else 2
    zrecvs, firsts = refs[:n], refs[n : n + 2]
    corners = refs[n + 2 : len(refs) - 11]
    out_u, out_v = refs[len(refs) - 11 : len(refs) - 9]
    U, V, DM, lam, mu, G, CI, F, KB = refs[len(refs) - 9 :]
    sides = plan.sides()
    Z, Y, X, H, T = plan.Z, plan.Y, plan.X, plan.H, plan.T
    PB, P0, R, ZB, ZS, YB = plan.PB, plan.P0, plan.hrow, plan.ZB, plan.ZS, plan.YB
    scal = place(plan)
    offset = scal[1]
    halves = range(H)
    row = lax.broadcasted_iota(jnp.int32, (8, LANES), 0)
    lane = lax.broadcasted_iota(jnp.int32, (8, LANES), 1)
    low_half = row < 4
    spare = (row == 3) | (row == 7)
    zero = jnp.zeros((8, LANES), f32)

    def shift_left(parts):
        rolled = [pltpu.roll(p, LANES - 1, 1) for p in parts] + [zero]
        return [jnp.where(lane == LANES - 1, rolled[h + 1], rolled[h]) for h in halves]

    def shift_right(parts):
        rolled = [zero] + [pltpu.roll(p, 1, 1) for p in parts]
        return [jnp.where(lane == 0, rolled[h], rolled[h + 1]) for h in halves]

    def columns(parts):
        ahead = shift_left(parts)
        tiles = []
        for h in halves:
            swapped = pltpu.roll(ahead[h], 4, 0)
            even = jnp.where(low_half, parts[h], swapped)
            odd = jnp.where(low_half, swapped, parts[h])
            high0 = even.astype(bf16).astype(f32)
            high1 = odd.astype(bf16).astype(f32)
            tiles.append(
                (
                    jnp.concatenate([high0, even - high0], 0).astype(bf16),
                    jnp.concatenate([high0, high1], 0).astype(bf16),
                    jnp.concatenate([high1, odd - high1], 0).astype(bf16),
                )
            )
        return tiles

    def put_columns(buffers, z, p, parts):
        for h, tiles in enumerate(columns(parts)):
            for j in range(3):
                for b in buffers:
                    KB[b, z, p, 16 * j : 16 * j + 16, h * LANES : (h + 1) * LANES] = tiles[j]

    mid = slice(R, R + 4 * Y)
    for z in range(Z):
        U[offset + z, :, mid, :] = xv[z, :, : 4 * Y, :]
        V[offset + z, :, mid, :] = xv[z, :, 4 * Y :, :]
    for zrecv, (at_u, at_v, lacks) in zip(zrecvs, halo_places(plan, scal)):
        for i in range(T):
            U[at_u + i, :, mid, :] = zrecv[i]
        for i in range(T - 1):
            V[at_v + i, :, mid, :] = zrecv[T + i]
    U[ZB:, :, :, :] = jnp.zeros((ZS - ZB, H, 4 * YB, LANES), f32)
    V[ZB:, :, :, :] = jnp.zeros((ZS - ZB, H, 4 * YB, LANES), f32)
    for s in range(T):
        G[s] = jnp.zeros((H, 4 * YB, LANES), f32)
        G[s, :, mid, :] = gown[s]
    own, waves = plan.own_tiles()
    for source, from_next in zip(firsts, sides):

        def write(kind, z, h, row, tile):
            (U if kind == "u" else V)[offset + z, h, pl.ds(row, 8), :] = tile

        take_halo(plan, own, source, 0, from_next, write)
        for t, (s, h, k, n_pairs) in enumerate(waves):
            at = aligned(jnp.where(from_next, R + 4 * Y, R - 8 * n_pairs) + 8 * k)
            G[s, h, pl.ds(at, 8), :] = source[len(own) + t]
    tiles = plan.corner_tiles()
    for k, (at_u, at_v, lacks) in enumerate(halo_places(plan, scal)):
        for source, from_next in zip(corners, sides):

            def write(kind, i, h, row, tile):
                if kind == "u":
                    U[at_u + i, h, pl.ds(row, 8), :] = tile
                else:
                    V[at_v + i - T, h, pl.ds(row, 8), :] = tile

            take_halo(plan, tiles, source, k * len(tiles), from_next, write)
        V[lacks, :, :, :] = jnp.zeros((H, 4 * YB, LANES), f32)

    n_levels = tables.shape[0] // 2

    def prepare(z, carry):
        for h in halves:
            for y in range(0, plan.YL, 8):
                count = min(8, YB - y)
                if count == 8:
                    level = U[z, h, pl.ds(4 * y + 3, 8, stride=4), :]
                    first = y
                else:
                    first = YB - 8
                    level = U[z, h, pl.ds(4 * first + 3, 8, stride=4), :]
                dil = jnp.zeros((8, LANES), f32)
                she = jnp.zeros((8, LANES), f32)
                for k in range(n_levels):
                    here = level == float(k + 1)
                    dil = jnp.where(here, tables[k], dil)
                    she = jnp.where(here, tables[n_levels + k], she)
                lam[z, h, first : first + 8, :] = dil
                mu[z, h, first : first + 8, :] = she
        for p in range(PB):
            at = slice(8 * p, 8 * p + 8)
            for h in halves:
                v = V[z, h, at, :]
                mass = jnp.where(
                    low_half,
                    jnp.broadcast_to(v[3:4, :], (8, LANES)),
                    jnp.broadcast_to(v[7:8, :], (8, LANES)),
                )
                DM[z, h, at, :] = jnp.where(spare, 0.0, time_step * mass)
            put_columns((0,), z, p, [U[z, h, at, :] for h in halves])
        for b in range(2):
            for p in range(widest_pair + 1 if b else PB, PB + 1):
                KB[b, z, p] = jnp.zeros((48, X), bf16)
        return carry

    widest_pair = (plan.hy + Y + T - 2) // 2
    lax.fori_loop(0, ZB, prepare, 0)
    for z in range(ZB, ZS):
        for b in range(2):
            KB[b, z] = jnp.zeros((PB + 1, 48, X), bf16)
        for ref in (DM, lam, mu):
            ref[z] = jnp.zeros(ref.shape[1:], f32)

    bottom = offset + Z - 1
    wave = tables[2 * n_levels]
    wave = jnp.where(scal[2] == 1, wave, zero)
    for h in halves:
        for p in range(PB):
            at = slice(8 * p, 8 * p + 8)
            CI[h, at, :] = wave * DM[bottom, h, at, :]

    def one_step(s, final):
        d = T - 1 - s
        cur, new = s % 2, 1 - s % 2
        p_first = (plan.hy - d - 1) // 2
        p_last = (plan.hy + Y - 1 + d) // 2
        if plan.D == 1:
            p_z0, count = 0, -(-Z // 2)
        elif plan.swap:
            top = scal[0] == 0
            count = -(-(Z + d + 1) // 2)
            p_z0 = jnp.where(top, 0, ZB - 2 * count)
        else:
            p_z0 = T - d - 1
            count = -(-(Z + 2 * d + 1) // 2)

        for p in range(p_first, p_last + 1):
            at = slice(8 * p, 8 * p + 8)
            for h in halves:
                v = V[bottom, h, at, :]
                V[bottom, h, at, :] = v + CI[h, at, :] * (G[s, h, at, :] - v)
        for p in range(p_first, p_last + 1):
            F[p] = jnp.zeros((2, H, 8, LANES), f32)

        def finish(z, p, g0, g1):
            at = slice(8 * p, 8 * p + 8)
            other = [
                pltpu.roll(jnp.where(low_half, g1[h], g0[h]), 4, 0) for h in halves
            ]
            other = shift_right(other)
            fresh = []
            for h in halves:
                force = jnp.where(low_half, g0[h], g1[h]) + other[h]
                v = V[z, h, at, :] - DM[z, h, at, :] * force
                u = U[z, h, at, :] + time_step * v
                V[z, h, at, :] = v
                U[z, h, at, :] = u
                fresh.append(u)
            if not final:
                put_columns((new,), z, p, fresh)

        def two_layers(i, carry):
            z0 = p_z0 + 2 * i
            side = [[zero for _ in halves] for _ in range(3)]
            for p in range(p_first, p_last + 1):
                right = jnp.concatenate(
                    [
                        KB[cur, z0, p],
                        KB[cur, z0, p + 1, :32],
                        KB[cur, z0 + 1, p],
                        KB[cur, z0 + 1, p + 1, :32],
                        KB[cur, z0 + 2, p],
                        KB[cur, z0 + 2, p + 1],
                    ],
                    0,
                )
                product = jnp.dot(weights[...], right, preferred_element_type=f32)
                node = [[None] * 3 for _ in range(3)]
                for zn in range(3):
                    node[zn][0] = side[zn]
                for y in range(2):
                    above = [F[p, y, h] for h in halves]
                    node[0][y] = above if y else [a + b for a, b in zip(node[0][0], above)]
                for ez in range(2):
                    for ey in range(2):
                        base = 64 * (2 * ez + ey)
                        y = 2 * p + ey
                        for h in halves:
                            lanes = slice(h * LANES, (h + 1) * LANES)
                            dil = jnp.broadcast_to(lam[z0 + ez, h, y : y + 1, :], (8, LANES))
                            she = jnp.broadcast_to(mu[z0 + ez, h, y : y + 1, :], (8, LANES))
                            for dz in range(2):
                                for dy in range(2):
                                    r = base + 8 * (2 * dz + dy)
                                    part = (
                                        dil * product[r : r + 8, lanes]
                                        + she * product[r + 32 : r + 40, lanes]
                                    )
                                    slot = node[ez + dz][ey + dy]
                                    if slot is None:
                                        slot = node[ez + dz][ey + dy] = [None] * H
                                    elif slot is side[ez + dz]:
                                        slot = node[ez + dz][ey + dy] = list(slot)
                                    slot[h] = part if slot[h] is None else slot[h] + part
                for y in range(2):
                    for h in halves:
                        F[p, y, h] = node[2][y][h]
                finish(z0, p, node[0][0], node[0][1])
                finish(z0 + 1, p, node[1][0], node[1][1])
                side = [node[zn][2] for zn in range(3)]
            return carry

        def chunk(first, rows):
            for i in range(rows):
                two_layers(first + i, 0)

        straight = count if plan.ZB <= 16 else 1
        full, rest = count // straight, count % straight
        lax.fori_loop(0, full * scal[3], lambda i, c: (chunk(straight * i, straight), c)[1], 0)
        assert rest == 0

    for s in range(T):
        one_step(s, s == T - 1)

    for z in range(Z):
        for h in halves:
            lanes = slice(h * LANES, (h + 1) * LANES)
            for y in range(0, Y, 8):
                for c in range(3):
                    at = pl.ds(R + 4 * y + c, 8, stride=4)
                    out_u[c, z, y : y + 8, lanes] = U[offset + z, h, at, :]
                    out_v[c, z, y : y + 8, lanes] = V[offset + z, h, at, :]


def smem():
    return pl.BlockSpec(memory_space=pltpu.SMEM)


def vmem():
    return pl.BlockSpec(memory_space=pltpu.VMEM)


def per_device(plan, u, v, m, mat, dilation_table, shear_table, stiffness_pair, impedance, mask, inc):
    Z, Y, X, H, T, D, L = plan.Z, plan.Y, plan.X, plan.H, plan.T, plan.D, plan.L
    shape = lambda *dims: jax.ShapeDtypeStruct(dims, f32)

    room = pltpu.CompilerParams(vmem_limit_bytes=40 * 2**20)
    rows, cols = selectors()
    n_tables = 2 * dilation_table.shape[0] + 1
    weights, tables = pl.pallas_call(
        matrix_kernel,
        out_shape=[pltpu.VMEM((256, 256), bf16), pltpu.VMEM((n_tables, 8, LANES), f32)],
        in_specs=[vmem()] * 3 + [smem()] * 3,
        out_specs=[vmem()] * 2,
        compiler_params=room,
        name="matrix",
    )(
        stiffness_pair.reshape(48, 24),
        jnp.asarray(rows, bf16),
        jnp.asarray(cols, bf16),
        dilation_table,
        shear_table,
        impedance,
    )

    n_sends = 0 if D == 1 else 1 if plan.swap else 2
    tiles, waves = plan.own_tiles()
    local = lambda *dims: pltpu.VMEM(dims, f32)
    edge = local(len(tiles) + len(waves), 8, LANES)
    packed = pl.pallas_call(
        lambda *refs: pack_kernel(plan, *refs),
        out_shape=[local(Z, H, 8 * Y, LANES), local(T, H, 4 * Y, LANES), edge, edge]
        + [local(2 * T - 1, H, 4 * Y, LANES)] * n_sends,
        in_specs=[vmem()] * 6,
        out_specs=[vmem()] * (4 + n_sends),
        compiler_params=room,
        name="pack",
    )(*[pltpu.with_memory_space_constraint(a, pltpu.HBM) for a in (u, v, m, mat, mask, inc)])
    xv, g, to_first, to_second = packed[:4]
    sends = packed[4:]

    def trade(array, start):
        pairs = [(i, i + 1) for i in range(start, L - 1, 2)]
        return lax.ppermute(array, "lat", pairs + [(j, i) for i, j in pairs])

    if D == 1:
        zrecvs = []
    elif plan.swap:
        zrecvs = [lax.ppermute(sends[0], "depth", [(0, 1), (1, 0)])]
    else:
        zrecvs = [
            lax.ppermute(sends[0], "depth", [(i, i + 1) for i in range(D - 1)]),
            lax.ppermute(sends[1], "depth", [(i + 1, i) for i in range(D - 1)]),
        ]
    firsts = [trade(to_first, 1), trade(to_second, 0)]
    corners = []
    if zrecvs:
        corner = local(len(zrecvs) * len(plan.corner_tiles()), 8, LANES)
        corner_first, corner_second = pl.pallas_call(
            lambda *refs: corner_kernel(plan, *refs),
            out_shape=[corner, corner],
            in_specs=[vmem()] * len(zrecvs),
            out_specs=[vmem()] * 2,
            compiler_params=room,
            name="corner",
        )(*[pltpu.with_memory_space_constraint(a, pltpu.VMEM) for a in zrecvs])
        corners = [trade(corner_first, 1), trade(corner_second, 0)]
    near = lambda arrays: [pltpu.with_memory_space_constraint(a, pltpu.VMEM) for a in arrays]
    zrecvs, corners = near(zrecvs), near(corners)
    first, second, xv, g, weights, tables = near([*firsts, xv, g, weights, tables])
    grid = (plan.ZS, H, 4 * plan.YB, LANES)
    new_u, new_v = pl.pallas_call(
        lambda *refs: main_kernel(plan, *refs),
        out_shape=[shape(3, Z, Y, X)] * 2,
        in_specs=[vmem()] * (6 + len(zrecvs) + len(corners)),
        out_specs=[vmem()] * 2,
        scratch_shapes=[
            pltpu.VMEM(grid, f32),
            pltpu.VMEM(grid, f32),
            pltpu.VMEM(grid, f32),
            pltpu.VMEM((plan.ZS, H, plan.YL, LANES), f32),
            pltpu.VMEM((plan.ZS, H, plan.YL, LANES), f32),
            pltpu.VMEM((T, H, 4 * plan.YB, LANES), f32),
            pltpu.VMEM((H, 4 * plan.YB, LANES), f32),
            pltpu.VMEM((plan.PB, 2, H, 8, LANES), f32),
            pltpu.VMEM((2, plan.ZS, plan.PB + 1, 48, X), bf16),
        ],
        compiler_params=room,
        name="steps",
    )(tables, weights, xv, g, *zrecvs, first, second, *corners)
    return new_u, new_v


def solution(mesh):
    field = P(None, "depth", "lat", None)
    in_specs = (
        field,
        field,
        P("depth", "lat", None),
        P("depth", "lat", None),
        P(),
        P(),
        P(),
        P(),
        P("lat", None),
        P(None, None, "lat", None),
    )

    def whole(displacement, *rest):
        plan = Plan(mesh, displacement, rest[-1])
        return jax.shard_map(
            lambda *args: per_device(plan, *args),
            mesh=mesh,
            in_specs=in_specs,
            out_specs=(field, field),
            check_vma=False,
        )(displacement, *rest)

    return whole
```

```python
import jax
import jax.numpy as jnp
import numpy as np
from jax import lax
from jax.experimental import pallas as pl
from jax.experimental.pallas import tpu as pltpu
from jax.sharding import PartitionSpec as P

time_step = 0.1
LANES = 128
f32 = jnp.float32
bf16 = jnp.bfloat16


class Plan:
    def __init__(self, mesh, displacement, incident):
        self.D = mesh.shape["depth"]
        self.L = mesh.shape["lat"]
        self.Z = displacement.shape[1] // self.D
        self.Y = displacement.shape[2] // self.L
        self.X = displacement.shape[3]
        self.H = self.X // LANES
        self.T = incident.shape[0]
        T = self.T
        assert T <= self.Z and T <= self.Y and self.Y % 8 == 0
        assert self.X % LANES == 0
        self.hy = T + T % 2
        self.YB = self.Y + 2 * self.hy
        self.PB = self.YB // 2
        self.P0 = self.hy // 2
        self.swap = self.D == 2
        self.ZB = self.Z + (0 if self.D == 1 else T if self.swap else 2 * T)
        self.ZS = self.ZB + 2
        self.gpairs = [-(-(T - 1 - s) // 2) for s in range(T)]
        self.hrow = 4 * self.hy

    def offset(self, depth):
        if self.D == 1:
            return 0
        return depth * self.T if self.swap else self.T

    def halo_tiles(self, u_layers, v_layers):
        n = self.hy // 2
        tiles = [("u", z, h, p) for z in u_layers for h in range(self.H) for p in range(n)]
        tiles += [("v", z, h, p) for z in v_layers for h in range(self.H) for p in range(n - 1)]
        if self.T % 2 == 0:
            tiles += [("half", z, h, 0) for z in v_layers for h in range(0, self.H, 2)]
        return tiles

    def own_tiles(self):
        return self.halo_tiles(range(self.Z), range(self.Z)), [
            (s, h, k, n_pairs)
            for s, n_pairs in enumerate(self.gpairs)
            for h in range(self.H)
            for k in range(n_pairs)
        ]

    def corner_tiles(self):
        return self.halo_tiles(range(self.T), range(self.T, 2 * self.T - 1))

    def sides(self):
        odd = lax.rem(lax.axis_index("lat"), jnp.int32(2))
        return odd == 1, odd == 0


def aligned(value):
    return pl.multiple_of(value, 8)


def first_half():
    return lax.broadcasted_iota(jnp.int32, (8, LANES), 0) < 4


def put_halo(plan, tiles, out, start, to_next, read):
    n, R, top = plan.hy // 2, plan.hrow, 4 * plan.Y - plan.hrow
    u_low = jnp.where(to_next, top, 0)
    v_low = jnp.where(to_next, top + 8, 0)
    far = jnp.where(to_next, top, R - 8)
    for t, (kind, z, h, p) in enumerate(tiles):
        if kind == "half":
            a, b = read("v", z, h, aligned(far)), read("v", z, h + 1, aligned(far))
            low = jnp.where(first_half(), a, pltpu.roll(b, 4, 0))
            high = jnp.where(first_half(), pltpu.roll(a, 4, 0), b)
            out[start + t] = jnp.where(to_next, high, low)
        else:
            out[start + t] = read(kind, z, h, aligned((u_low if kind == "u" else v_low) + 8 * p))


def take_halo(plan, tiles, source, start, from_next, write):
    n, R = plan.hy // 2, plan.hrow
    u_low = jnp.where(from_next, R + 4 * plan.Y, 0)
    v_low = jnp.where(from_next, R + 4 * plan.Y, 8)
    far = jnp.where(from_next, R + 4 * plan.Y + 8 * (n - 1), 0)
    for t, (kind, z, h, p) in enumerate(tiles):
        tile = source[start + t]
        if kind == "half":
            turned = pltpu.roll(tile, 4, 0)
            keep = first_half() == from_next
            write("v", z, h, aligned(far), jnp.where(keep, jnp.where(from_next, tile, turned), 0.0))
            write("v", z, h + 1, aligned(far), jnp.where(keep, jnp.where(from_next, turned, tile), 0.0))
        else:
            write(kind, z, h, aligned((u_low if kind == "u" else v_low) + 8 * p), tile)


def selectors():
    rows = np.zeros((4, 64, 48), np.float32)
    cols = np.zeros((2, 4, 24, 240), np.float32)

    def half(parity, dx):
        return 4 * (dx ^ parity)

    blocks = [(0, 0, 0), (8, 0, 0), (16, 0, 1), (24, 1, 1), (32, 1, 0), (40, 1, 0), (48, 2, 0), (56, 2, 0), (64, 2, 1)]
    for ez in range(2):
        for ey in range(2):
            e = 2 * ez + ey
            for lm in range(2):
                for dz in range(2):
                    for dy in range(2):
                        for dx in range(2):
                            for c in range(3):
                                dof = (4 * dz + 2 * dy + dx) * 3 + c
                                r = half((ey + dy) % 2, dx) + c
                                rows[e, ((lm * 2 + dz) * 2 + dy) * 8 + r, lm * 24 + dof] = 1
            for base, node, low in blocks:
                for zn in range(3):
                    dz, dy = zn - ez, node - ey
                    if dz in (0, 1) and dy in (0, 1):
                        for dx in range(2):
                            for c in range(3):
                                dof = (4 * dz + 2 * dy + dx) * 3 + c
                                cols[low, e, dof, zn * 80 + base + half(node % 2, dx) + c] = 1
    return rows, cols


def matrix_kernel(stiff_ref, rows_ref, cols_ref, dilations, shears, imp, out_ref, tiles_ref):
    stiff = stiff_ref[...]
    high = stiff.astype(bf16)
    low = (stiff - high.astype(f32)).astype(bf16)
    for e in range(4):
        total = None
        for part, k in ((high, 0), (low, 1)):
            picked = jnp.dot(rows_ref[e], part, preferred_element_type=f32).astype(bf16)
            placed = jnp.dot(picked, cols_ref[k, e], preferred_element_type=f32)
            total = placed if total is None else total + placed
        out_ref[64 * e : 64 * e + 64, :] = total.astype(bf16)
    n = dilations.shape[0]
    for k in range(n):
        tiles_ref[k] = jnp.full((8, LANES), dilations[k], f32)
        tiles_ref[n + k] = jnp.full((8, LANES), shears[k], f32)
    row = lax.broadcasted_iota(jnp.int32, (8, LANES), 0)
    wave = jnp.zeros((8, LANES), f32)
    for c in range(3):
        wave = jnp.where((row == c) | (row == 4 + c), imp[c], wave)
    tiles_ref[2 * n] = wave


def pack_kernel(plan, u, v, m, mat, mask, inc, xv, g, to_first, to_second, *zsends):
    Z, Y, H, T = plan.Z, plan.Y, plan.H, plan.T
    scal = place(plan)
    for z in range(Z):
        for h in range(H):
            lanes = slice(h * LANES, (h + 1) * LANES)
            for y in range(0, Y, 8):
                rows = slice(y, y + 8)
                for c in range(3):
                    xv[z, h, pl.ds(4 * y + c, 8, stride=4), :] = u[c, z, rows, lanes]
                    xv[z, h, pl.ds(4 * (Y + y) + c, 8, stride=4), :] = v[c, z, rows, lanes]
                xv[z, h, pl.ds(4 * y + 3, 8, stride=4), :] = mat[z, rows, lanes].astype(f32) + 1.0
                xv[z, h, pl.ds(4 * (Y + y) + 3, 8, stride=4), :] = m[z, rows, lanes]
    for h in range(H):
        lanes = slice(h * LANES, (h + 1) * LANES)
        for y in range(0, Y, 8):
            rows = slice(y, y + 8)
            double = 2.0 * mask[rows, lanes].astype(f32)
            for s in range(T):
                for c in range(3):
                    g[s, h, pl.ds(4 * y + c, 8, stride=4), :] = double * inc[s, c, rows, lanes]
                g[s, h, pl.ds(4 * y + 3, 8, stride=4), :] = jnp.zeros((8, LANES), f32)
    tiles, waves = plan.own_tiles()

    def read(kind, z, h, row):
        return xv[z, h, pl.ds(row + (4 * Y if kind == "v" else 0), 8), :]

    for out, to_next in zip((to_first, to_second), plan.sides()):
        put_halo(plan, tiles, out, 0, to_next, read)
        for t, (s, h, k, n_pairs) in enumerate(waves):
            at = aligned(jnp.where(to_next, 4 * Y - 8 * n_pairs, 0) + 8 * k)
            out[len(tiles) + t] = g[s, h, pl.ds(at, 8), :]
    for k, zsend in enumerate(zsends):
        if plan.swap:
            first = jnp.where(scal[0] == 0, Z - T, 0)
            first_v = jnp.where(scal[0] == 0, Z - T + 1, 0)
        else:
            first, first_v = (Z - T, Z - T + 1) if k == 0 else (0, 0)
        for i in range(T):
            zsend[i] = xv[first + i, :, : 4 * Y, :]
        for i in range(T - 1):
            zsend[T + i] = xv[first_v + i, :, 4 * Y :, :]


def place(plan):
    depth = lax.axis_index("depth")
    one = (depth >= 0).astype(jnp.int32)
    return depth, plan.offset(depth), (depth == plan.D - 1).astype(jnp.int32), one


def halo_places(plan, scal):
    if plan.D == 1:
        return []
    if plan.swap:
        top = scal[0] == 0
        return [
            (
                jnp.where(top, plan.Z, 0),
                jnp.where(top, plan.Z, 1),
                jnp.where(top, plan.Z + plan.T - 1, 0),
            )
        ]
    last = plan.T + plan.Z
    return [(0, 1, 0), (last, last, last + plan.T - 1)]


def corner_kernel(plan, *refs):
    n = len(refs) - 2
    zrecvs, outs = refs[:n], refs[n:]
    tiles = plan.corner_tiles()
    for out, to_next in zip(outs, plan.sides()):
        for k, zrecv in enumerate(zrecvs):

            def read(kind, i, h, row):
                return zrecv[i, h, pl.ds(row, 8), :]

            put_halo(plan, tiles, out, k * len(tiles), to_next, read)


def column_tiles(plan, parts):
    ahead = shift_left(plan, parts)
    tiles = []
    for h in range(plan.H):
        swapped = pltpu.roll(ahead[h], 4, 0)
        even = jnp.where(first_half(), parts[h], swapped)
        odd = jnp.where(first_half(), swapped, parts[h])
        high0 = even.astype(bf16).astype(f32)
        high1 = odd.astype(bf16).astype(f32)
        tiles.append(
            (
                jnp.concatenate([high0, even - high0], 0).astype(bf16),
                jnp.concatenate([high0, high1], 0).astype(bf16),
                jnp.concatenate([high1, odd - high1], 0).astype(bf16),
            )
        )
    return tiles


def put_columns(plan, columns, z, p, parts):
    for h, tiles in enumerate(column_tiles(plan, parts)):
        for j in range(3):
            columns[z, p, 16 * j : 16 * j + 16, h * LANES : (h + 1) * LANES] = tiles[j]


def shift_left(plan, parts):
    lane = lax.broadcasted_iota(jnp.int32, (8, LANES), 1)
    rolled = [pltpu.roll(p, LANES - 1, 1) for p in parts] + [jnp.zeros((8, LANES), f32)]
    return [jnp.where(lane == LANES - 1, rolled[h + 1], rolled[h]) for h in range(plan.H)]


def shift_right(plan, parts):
    lane = lax.broadcasted_iota(jnp.int32, (8, LANES), 1)
    rolled = [jnp.zeros((8, LANES), f32)] + [pltpu.roll(p, 1, 1) for p in parts]
    return [jnp.where(lane == 0, rolled[h], rolled[h + 1]) for h in range(plan.H)]


def prepare(plan, tables, U, V, DM, lam, mu, columns, z, pairs, level_rows):
    n_levels = tables.shape[0] // 2
    row = lax.broadcasted_iota(jnp.int32, (8, LANES), 0)
    spare = (row == 3) | (row == 7)
    for h in range(plan.H):
        for first in level_rows:
            level = U[z, h, pl.ds(4 * first + 3, 8, stride=4), :]
            dil = jnp.zeros((8, LANES), f32)
            she = jnp.zeros((8, LANES), f32)
            for k in range(n_levels):
                here = level == float(k + 1)
                dil = jnp.where(here, tables[k], dil)
                she = jnp.where(here, tables[n_levels + k], she)
            lam[z, h, first : first + 8, :] = dil
            mu[z, h, first : first + 8, :] = she
    for p in pairs:
        at = slice(8 * p, 8 * p + 8)
        for h in range(plan.H):
            v = V[z, h, at, :]
            mass = jnp.where(
                first_half(),
                jnp.broadcast_to(v[3:4, :], (8, LANES)),
                jnp.broadcast_to(v[7:8, :], (8, LANES)),
            )
            DM[z, h, at, :] = jnp.where(spare, 0.0, time_step * mass)
        put_columns(plan, columns, z, p, [U[z, h, at, :] for h in range(plan.H)])


def begin_kernel(plan, tables, xv, gown, *refs):
    n = len(refs) - 9
    zrecvs, firsts = refs[:n], refs[n : n + 2]
    U, V, DM, lam, mu, G, columns = refs[n + 2 :]
    Z, Y, X, H, T = plan.Z, plan.Y, plan.X, plan.H, plan.T
    PB, P0, R, ZB, ZS, YB = plan.PB, plan.P0, plan.hrow, plan.ZB, plan.ZS, plan.YB
    scal = place(plan)
    offset = scal[1]
    sides = plan.sides()
    mid = slice(R, R + 4 * Y)
    for z in range(Z):
        U[offset + z, :, mid, :] = xv[z, :, : 4 * Y, :]
        V[offset + z, :, mid, :] = xv[z, :, 4 * Y :, :]
    for zrecv, (at_u, at_v, lacks) in zip(zrecvs, halo_places(plan, scal)):
        for i in range(T):
            U[at_u + i, :, mid, :] = zrecv[i]
        for i in range(T - 1):
            V[at_v + i, :, mid, :] = zrecv[T + i]
        V[lacks, :, :, :] = jnp.zeros((H, 4 * YB, LANES), f32)
    for s in range(T):
        G[s] = jnp.zeros((H, 4 * YB, LANES), f32)
        G[s, :, mid, :] = gown[s]
    own, waves = plan.own_tiles()
    for source, from_next in zip(firsts, sides):

        def write(kind, z, h, row, tile):
            (U if kind == "u" else V)[offset + z, h, pl.ds(row, 8), :] = tile

        take_halo(plan, own, source, 0, from_next, write)
        for t, (s, h, k, n_pairs) in enumerate(waves):
            at = aligned(jnp.where(from_next, R + 4 * Y, R - 8 * n_pairs) + 8 * k)
            G[s, h, pl.ds(at, 8), :] = source[len(own) + t]

    def own_layer(z, carry):
        rows = [*range(0, YB - 7, 8), YB - 8]
        prepare(plan, tables, U, V, DM, lam, mu, columns, offset + z, range(PB), sorted(set(rows)))
        columns[offset + z, PB] = jnp.zeros((48, X), bf16)
        return carry

    lax.fori_loop(0, Z, own_layer, 0)
    for at_u, at_v, lacks in halo_places(plan, scal):

        def halo_layer(i, carry):
            rows = range(plan.hy, plan.hy + Y, 8)
            prepare(plan, tables, U, V, DM, lam, mu, columns, at_u + i, range(P0, P0 + Y // 2), rows)
            columns[at_u + i, PB] = jnp.zeros((48, X), bf16)
            return carry

        lax.fori_loop(0, T, halo_layer, 0)
    for z in range(ZB, ZS):
        for ref in (U, V, DM, lam, mu, columns):
            ref[z] = jnp.zeros(ref.shape[1:], ref.dtype)


def main_kernel(plan, tables, weights, *refs):
    corners = refs[: len(refs) - 18]
    G = refs[len(refs) - 13]
    out_u, out_v, U, V, DM, lam, mu, columns, CI, F, spare_columns = refs[len(refs) - 11 :]
    Z, Y, X, H, T = plan.Z, plan.Y, plan.X, plan.H, plan.T
    PB, P0, R, ZB, ZS, YB = plan.PB, plan.P0, plan.hrow, plan.ZB, plan.ZS, plan.YB
    scal = place(plan)
    offset = scal[1]
    sides = plan.sides()
    halves = range(H)
    n_levels = tables.shape[0] // 2
    low_half = first_half()
    zero = jnp.zeros((8, LANES), f32)

    tiles = plan.corner_tiles()
    for k, (at_u, at_v, lacks) in enumerate(halo_places(plan, scal)):
        for source, from_next in zip(corners, sides):

            def write(kind, i, h, row, tile):
                if kind == "u":
                    U[at_u + i, h, pl.ds(row, 8), :] = tile
                else:
                    V[at_v + i - T, h, pl.ds(row, 8), :] = tile

            take_halo(plan, tiles, source, k * len(tiles), from_next, write)

        def halo_layer(i, carry):
            pairs = [*range(P0), *range(P0 + Y // 2, PB)]
            prepare(plan, tables, U, V, DM, lam, mu, columns, at_u + i, pairs, (0, YB - 8))
            return carry

        lax.fori_loop(0, T, halo_layer, 0)
    widest_pair = (plan.hy + Y + T - 2) // 2
    for z in range(ZS):
        for p in range(widest_pair + 1 if z < ZB else 0, PB + 1):
            spare_columns[z, p] = jnp.zeros((48, X), bf16)

    bottom = offset + Z - 1
    wave = tables[2 * n_levels]
    wave = jnp.where(scal[2] == 1, wave, zero)
    for h in halves:
        for p in range(PB):
            at = slice(8 * p, 8 * p + 8)
            CI[h, at, :] = wave * DM[bottom, h, at, :]

    def one_step(s, final):
        d = T - 1 - s
        cur, new = (columns, spare_columns)[:: 1 - 2 * (s % 2)]
        p_first = (plan.hy - d - 1) // 2
        p_last = (plan.hy + Y - 1 + d) // 2
        if plan.D == 1:
            p_z0, count = 0, -(-Z // 2)
        elif plan.swap:
            top = scal[0] == 0
            count = -(-(Z + d + 1) // 2)
            p_z0 = jnp.where(top, 0, ZB - 2 * count)
        else:
            p_z0 = T - d - 1
            count = -(-(Z + 2 * d + 1) // 2)

        for p in range(p_first, p_last + 1):
            at = slice(8 * p, 8 * p + 8)
            for h in halves:
                v = V[bottom, h, at, :]
                V[bottom, h, at, :] = v + CI[h, at, :] * (G[s, h, at, :] - v)
        for p in range(p_first, p_last + 1):
            F[p] = jnp.zeros((2, H, 8, LANES), f32)

        def finish(z, p, g0, g1):
            at = slice(8 * p, 8 * p + 8)
            other = [
                pltpu.roll(jnp.where(low_half, g1[h], g0[h]), 4, 0) for h in halves
            ]
            other = shift_right(plan, other)
            fresh = []
            for h in halves:
                force = jnp.where(low_half, g0[h], g1[h]) + other[h]
                v = V[z, h, at, :] - DM[z, h, at, :] * force
                u = U[z, h, at, :] + time_step * v
                V[z, h, at, :] = v
                U[z, h, at, :] = u
                fresh.append(u)
            if not final:
                put_columns(plan, new, z, p, fresh)

        def two_layers(i, carry):
            z0 = p_z0 + 2 * i
            side = [[zero for _ in halves] for _ in range(3)]
            for p in range(p_first, p_last + 1):
                right = jnp.concatenate(
                    [
                        cur[z0, p],
                        cur[z0, p + 1, :32],
                        cur[z0 + 1, p],
                        cur[z0 + 1, p + 1, :32],
                        cur[z0 + 2, p],
                        cur[z0 + 2, p + 1, :32],
                    ],
                    0,
                )
                product = jnp.dot(weights[...], right, preferred_element_type=f32)
                node = [[None] * 3 for _ in range(3)]
                for zn in range(3):
                    node[zn][0] = side[zn]
                for y in range(2):
                    above = [F[p, y, h] for h in halves]
                    node[0][y] = above if y else [a + b for a, b in zip(node[0][0], above)]
                for ez in range(2):
                    for ey in range(2):
                        base = 64 * (2 * ez + ey)
                        y = 2 * p + ey
                        for h in halves:
                            lanes = slice(h * LANES, (h + 1) * LANES)
                            dil = jnp.broadcast_to(lam[z0 + ez, h, y : y + 1, :], (8, LANES))
                            she = jnp.broadcast_to(mu[z0 + ez, h, y : y + 1, :], (8, LANES))
                            for dz in range(2):
                                for dy in range(2):
                                    r = base + 8 * (2 * dz + dy)
                                    part = (
                                        dil * product[r : r + 8, lanes]
                                        + she * product[r + 32 : r + 40, lanes]
                                    )
                                    slot = node[ez + dz][ey + dy]
                                    if slot is None:
                                        slot = node[ez + dz][ey + dy] = [None] * H
                                    elif slot is side[ez + dz]:
                                        slot = node[ez + dz][ey + dy] = list(slot)
                                    slot[h] = part if slot[h] is None else slot[h] + part
                for y in range(2):
                    for h in halves:
                        F[p, y, h] = node[2][y][h]
                finish(z0, p, node[0][0], node[0][1])
                finish(z0 + 1, p, node[1][0], node[1][1])
                side = [node[zn][2] for zn in range(3)]
            return carry

        def chunk(first, rows):
            for i in range(rows):
                two_layers(first + i, 0)

        straight = count if plan.ZB <= 16 else 1
        full, rest = count // straight, count % straight
        lax.fori_loop(0, full * scal[3], lambda i, c: (chunk(straight * i, straight), c)[1], 0)
        assert rest == 0

    for s in range(T):
        one_step(s, s == T - 1)

    for z in range(Z):
        for h in halves:
            lanes = slice(h * LANES, (h + 1) * LANES)
            for y in range(0, Y, 8):
                for c in range(3):
                    at = pl.ds(R + 4 * y + c, 8, stride=4)
                    out_u[c, z, y : y + 8, lanes] = U[offset + z, h, at, :]
                    out_v[c, z, y : y + 8, lanes] = V[offset + z, h, at, :]


def smem():
    return pl.BlockSpec(memory_space=pltpu.SMEM)


def vmem():
    return pl.BlockSpec(memory_space=pltpu.VMEM)


def per_device(plan, u, v, m, mat, dilation_table, shear_table, stiffness_pair, impedance, mask, inc):
    Z, Y, X, H, T, D, L = plan.Z, plan.Y, plan.X, plan.H, plan.T, plan.D, plan.L
    shape = lambda *dims: jax.ShapeDtypeStruct(dims, f32)

    room = pltpu.CompilerParams(vmem_limit_bytes=40 * 2**20)
    rows, cols = selectors()
    n_tables = 2 * dilation_table.shape[0] + 1
    weights, tables = pl.pallas_call(
        matrix_kernel,
        out_shape=[pltpu.VMEM((256, 240), bf16), pltpu.VMEM((n_tables, 8, LANES), f32)],
        in_specs=[vmem()] * 3 + [smem()] * 3,
        out_specs=[vmem()] * 2,
        compiler_params=room,
        name="matrix",
    )(
        *[
            pltpu.with_memory_space_constraint(a, pltpu.HBM)
            for a in (
                stiffness_pair.reshape(48, 24),
                jnp.asarray(rows, bf16),
                jnp.asarray(cols, bf16),
                dilation_table,
                shear_table,
                impedance,
            )
        ]
    )

    n_sends = 0 if D == 1 else 1 if plan.swap else 2
    tiles, waves = plan.own_tiles()
    local = lambda *dims: pltpu.VMEM(dims, f32)
    edge = local(len(tiles) + len(waves), 8, LANES)
    packed = pl.pallas_call(
        lambda *refs: pack_kernel(plan, *refs),
        out_shape=[local(Z, H, 8 * Y, LANES), local(T, H, 4 * Y, LANES), edge, edge]
        + [local(2 * T - 1, H, 4 * Y, LANES)] * n_sends,
        in_specs=[vmem()] * 6,
        out_specs=[vmem()] * (4 + n_sends),
        compiler_params=room,
        name="pack",
    )(*[pltpu.with_memory_space_constraint(a, pltpu.HBM) for a in (u, v, m, mat, mask, inc)])
    xv, g, to_first, to_second = packed[:4]
    sends = packed[4:]

    def trade(array, start):
        pairs = [(i, i + 1) for i in range(start, L - 1, 2)]
        return lax.ppermute(array, "lat", pairs + [(j, i) for i, j in pairs])

    if D == 1:
        zrecvs = []
    elif plan.swap:
        zrecvs = [lax.ppermute(sends[0], "depth", [(0, 1), (1, 0)])]
    else:
        zrecvs = [
            lax.ppermute(sends[0], "depth", [(i, i + 1) for i in range(D - 1)]),
            lax.ppermute(sends[1], "depth", [(i + 1, i) for i in range(D - 1)]),
        ]
    firsts = [trade(to_first, 1), trade(to_second, 0)]
    corners = []
    if zrecvs:
        corner = local(len(zrecvs) * len(plan.corner_tiles()), 8, LANES)
        corner_first, corner_second = pl.pallas_call(
            lambda *refs: corner_kernel(plan, *refs),
            out_shape=[corner, corner],
            in_specs=[vmem()] * len(zrecvs),
            out_specs=[vmem()] * 2,
            compiler_params=room,
            name="corner",
        )(*[pltpu.with_memory_space_constraint(a, pltpu.VMEM) for a in zrecvs])
        corners = [trade(corner_first, 1), trade(corner_second, 0)]
    near = lambda arrays: [pltpu.with_memory_space_constraint(a, pltpu.VMEM) for a in arrays]
    grid = (plan.ZS, H, 4 * plan.YB, LANES)
    moduli = (plan.ZS, H, plan.YB, LANES)
    held = (plan.ZS, plan.PB + 1, 48, X)
    state = [local(*grid), local(*grid), local(*grid), local(*moduli), local(*moduli)]
    columns = pltpu.VMEM(held, bf16)
    begun = pl.pallas_call(
        lambda *refs: begin_kernel(plan, *refs),
        out_shape=[*state, local(T, H, 4 * plan.YB, LANES), columns],
        in_specs=[vmem()] * (5 + len(zrecvs)),
        out_specs=[vmem()] * 7,
        compiler_params=room,
        name="begin",
    )(*near([tables, xv, g, *zrecvs, *firsts]))
    *state_in, waves_in, columns_in = near(begun)
    n = 2 + len(corners)
    new_u, new_v, *_ = pl.pallas_call(
        lambda *refs: main_kernel(plan, *refs),
        out_shape=[shape(3, Z, Y, X), shape(3, Z, Y, X), *state, columns],
        in_specs=[vmem()] * (n + 7),
        out_specs=[vmem()] * 8,
        input_output_aliases={n + i: 2 + i for i in range(5)} | {n + 6: 7},
        scratch_shapes=[
            pltpu.VMEM((H, 4 * plan.YB, LANES), f32),
            pltpu.VMEM((plan.PB, 2, H, 8, LANES), f32),
            pltpu.VMEM(held, bf16),
        ],
        compiler_params=room,
        name="steps",
    )(*near([tables, weights, *corners]), *state_in, waves_in, columns_in)
    return new_u, new_v


def solution(mesh):
    field = P(None, "depth", "lat", None)
    in_specs = (
        field,
        field,
        P("depth", "lat", None),
        P("depth", "lat", None),
        P(),
        P(),
        P(),
        P(),
        P("lat", None),
        P(None, None, "lat", None),
    )

    def whole(displacement, *rest):
        plan = Plan(mesh, displacement, rest[-1])
        return jax.shard_map(
            lambda *args: per_device(plan, *args),
            mesh=mesh,
            in_specs=in_specs,
            out_specs=(field, field),
            check_vma=False,
        )(displacement, *rest)

    return whole
```

```python
import jax
import jax.numpy as jnp
import numpy as np
from jax import lax
from jax.experimental import pallas as pl
from jax.experimental.pallas import tpu as pltpu
from jax.sharding import PartitionSpec as P

time_step = 0.1
LANES = 128
f32 = jnp.float32
bf16 = jnp.bfloat16


class Plan:
    def __init__(self, mesh, displacement, incident):
        self.D = mesh.shape["depth"]
        self.L = mesh.shape["lat"]
        self.Z = displacement.shape[1] // self.D
        self.Y = displacement.shape[2] // self.L
        self.X = displacement.shape[3]
        self.H = self.X // LANES
        self.T = incident.shape[0]
        T = self.T
        assert T <= self.Z and T <= self.Y and self.Y % 8 == 0
        assert self.X % LANES == 0
        self.hy = T + T % 2
        self.YB = self.Y + 2 * self.hy
        self.PB = self.YB // 2
        self.P0 = self.hy // 2
        self.swap = self.D == 2
        self.ZB = self.Z + (0 if self.D == 1 else T if self.swap else 2 * T)
        self.ZS = self.ZB + 2
        self.gpairs = [-(-(T - 1 - s) // 2) for s in range(T)]
        self.hrow = 4 * self.hy

    def offset(self, depth):
        if self.D == 1:
            return 0
        return depth * self.T if self.swap else self.T

    def halo_tiles(self, u_layers, v_layers):
        n = self.hy // 2
        tiles = [("u", z, h, p) for z in u_layers for h in range(self.H) for p in range(n)]
        tiles += [("v", z, h, p) for z in v_layers for h in range(self.H) for p in range(n - 1)]
        if self.T % 2 == 0:
            tiles += [("half", z, h, 0) for z in v_layers for h in range(0, self.H, 2)]
        return tiles

    def own_tiles(self):
        return self.halo_tiles(range(self.Z), range(self.Z)), [
            (s, h, k, n_pairs)
            for s, n_pairs in enumerate(self.gpairs)
            for h in range(self.H)
            for k in range(n_pairs)
        ]

    def corner_tiles(self):
        return self.halo_tiles(range(self.T), range(self.T, 2 * self.T - 1))

    def sides(self):
        odd = lax.rem(lax.axis_index("lat"), jnp.int32(2))
        return odd == 1, odd == 0


def aligned(value):
    return pl.multiple_of(value, 8)


def first_half():
    return lax.broadcasted_iota(jnp.int32, (8, LANES), 0) < 4


def put_halo(plan, tiles, out, start, to_next, read):
    n, R, top = plan.hy // 2, plan.hrow, 4 * plan.Y - plan.hrow
    u_low = jnp.where(to_next, top, 0)
    v_low = jnp.where(to_next, top + 8, 0)
    far = jnp.where(to_next, top, R - 8)
    for t, (kind, z, h, p) in enumerate(tiles):
        if kind == "half":
            a, b = read("v", z, h, aligned(far)), read("v", z, h + 1, aligned(far))
            low = jnp.where(first_half(), a, pltpu.roll(b, 4, 0))
            high = jnp.where(first_half(), pltpu.roll(a, 4, 0), b)
            out[start + t] = jnp.where(to_next, high, low)
        else:
            out[start + t] = read(kind, z, h, aligned((u_low if kind == "u" else v_low) + 8 * p))


def take_halo(plan, tiles, source, start, from_next, write):
    n, R = plan.hy // 2, plan.hrow
    u_low = jnp.where(from_next, R + 4 * plan.Y, 0)
    v_low = jnp.where(from_next, R + 4 * plan.Y, 8)
    far = jnp.where(from_next, R + 4 * plan.Y + 8 * (n - 1), 0)
    for t, (kind, z, h, p) in enumerate(tiles):
        tile = source[start + t]
        if kind == "half":
            turned = pltpu.roll(tile, 4, 0)
            keep = first_half() == from_next
            write("v", z, h, aligned(far), jnp.where(keep, jnp.where(from_next, tile, turned), 0.0))
            write("v", z, h + 1, aligned(far), jnp.where(keep, jnp.where(from_next, turned, tile), 0.0))
        else:
            write(kind, z, h, aligned((u_low if kind == "u" else v_low) + 8 * p), tile)


def selectors():
    rows = np.zeros((4, 64, 48), np.float32)

    def half(parity, dx):
        return 4 * (dx ^ parity)

    blocks = [(0, 0, 0), (8, 0, 0), (16, 0, 1), (24, 1, 1), (32, 1, 0), (40, 1, 0), (48, 2, 0), (56, 2, 0), (64, 2, 1)]
    for ez in range(2):
        for ey in range(2):
            for lm in range(2):
                for dz in range(2):
                    for dy in range(2):
                        for dx in range(2):
                            for c in range(3):
                                dof = (4 * dz + 2 * dy + dx) * 3 + c
                                r = half((ey + dy) % 2, dx) + c
                                rows[2 * ez + ey, ((lm * 2 + dz) * 2 + dy) * 8 + r, lm * 24 + dof] = 1
    cols = []
    for layers, eys, (start, stop) in VARIANTS:
        width = stop - start
        elements = [(ez, ey) for ez in range(layers) for ey in eys]
        part = np.zeros((2, len(elements), 24, (layers + 1) * width), np.float32)
        for e, (ez, ey) in enumerate(elements):
            for base, node, low in blocks:
                for zn in range(layers + 1):
                    dz, dy = zn - ez, node - ey
                    if dz in (0, 1) and dy in (0, 1):
                        assert start <= base < stop
                        for dx in range(2):
                            for c in range(3):
                                dof = (4 * dz + 2 * dy + dx) * 3 + c
                                part[low, e, dof, zn * width + base - start + half(node % 2, dx) + c] = 1
        cols.append(part)
    return rows, cols


VARIANTS = [(n, eys, span) for n in (2, 1) for eys, span in (((0, 1), (0, 80)), ((0,), (0, 48)), ((1,), (16, 80)))]


def matrix_kernel(stiff_ref, rows_ref, dilations, shears, imp, *refs):
    cols_refs, out_refs, tiles_ref = refs[: len(VARIANTS)], refs[len(VARIANTS) : -1], refs[-1]
    stiff = stiff_ref[...]
    high = stiff.astype(bf16)
    low = (stiff - high.astype(f32)).astype(bf16)
    picked = [
        [jnp.dot(rows_ref[e], part, preferred_element_type=f32).astype(bf16) for part in (high, low)]
        for e in range(4)
    ]
    for (layers, eys, _), cols_ref, out_ref in zip(VARIANTS, cols_refs, out_refs):
        elements = [2 * ez + ey for ez in range(layers) for ey in eys]
        for i, e in enumerate(elements):
            total = None
            for k in range(2):
                placed = jnp.dot(picked[e][k], cols_ref[k, i], preferred_element_type=f32)
                total = placed if total is None else total + placed
            out_ref[64 * i : 64 * i + 64, :] = total.astype(bf16)
    n = dilations.shape[0]
    for k in range(n):
        tiles_ref[k] = jnp.full((8, LANES), dilations[k], f32)
        tiles_ref[n + k] = jnp.full((8, LANES), shears[k], f32)
    row = lax.broadcasted_iota(jnp.int32, (8, LANES), 0)
    wave = jnp.zeros((8, LANES), f32)
    for c in range(3):
        wave = jnp.where((row == c) | (row == 4 + c), imp[c], wave)
    tiles_ref[2 * n] = wave


def pack_kernel(plan, u, v, m, mat, mask, inc, xv, g, to_first, to_second, *zsends):
    Z, Y, H, T = plan.Z, plan.Y, plan.H, plan.T
    scal = place(plan)
    for z in range(Z):
        for h in range(H):
            lanes = slice(h * LANES, (h + 1) * LANES)
            for y in range(0, Y, 8):
                rows = slice(y, y + 8)
                for c in range(3):
                    xv[z, h, pl.ds(4 * y + c, 8, stride=4), :] = u[c, z, rows, lanes]
                    xv[z, h, pl.ds(4 * (Y + y) + c, 8, stride=4), :] = v[c, z, rows, lanes]
                xv[z, h, pl.ds(4 * y + 3, 8, stride=4), :] = mat[z, rows, lanes].astype(f32) + 1.0
                xv[z, h, pl.ds(4 * (Y + y) + 3, 8, stride=4), :] = m[z, rows, lanes]
    for h in range(H):
        lanes = slice(h * LANES, (h + 1) * LANES)
        for y in range(0, Y, 8):
            rows = slice(y, y + 8)
            double = 2.0 * mask[rows, lanes].astype(f32)
            for s in range(T):
                for c in range(3):
                    g[s, h, pl.ds(4 * y + c, 8, stride=4), :] = double * inc[s, c, rows, lanes]
                g[s, h, pl.ds(4 * y + 3, 8, stride=4), :] = jnp.zeros((8, LANES), f32)
    tiles, waves = plan.own_tiles()

    def read(kind, z, h, row):
        return xv[z, h, pl.ds(row + (4 * Y if kind == "v" else 0), 8), :]

    for out, to_next in zip((to_first, to_second), plan.sides()):
        put_halo(plan, tiles, out, 0, to_next, read)
        for t, (s, h, k, n_pairs) in enumerate(waves):
            at = aligned(jnp.where(to_next, 4 * Y - 8 * n_pairs, 0) + 8 * k)
            out[len(tiles) + t] = g[s, h, pl.ds(at, 8), :]
    for k, zsend in enumerate(zsends):
        if plan.swap:
            first = jnp.where(scal[0] == 0, Z - T, 0)
            first_v = jnp.where(scal[0] == 0, Z - T + 1, 0)
        else:
            first, first_v = (Z - T, Z - T + 1) if k == 0 else (0, 0)
        for i in range(T):
            zsend[i] = xv[first + i, :, : 4 * Y, :]
        for i in range(T - 1):
            zsend[T + i] = xv[first_v + i, :, 4 * Y :, :]


def place(plan):
    depth = lax.axis_index("depth")
    one = (depth >= 0).astype(jnp.int32)
    return depth, plan.offset(depth), (depth == plan.D - 1).astype(jnp.int32), one


def halo_places(plan, scal):
    if plan.D == 1:
        return []
    if plan.swap:
        top = scal[0] == 0
        return [
            (
                jnp.where(top, plan.Z, 0),
                jnp.where(top, plan.Z, 1),
                jnp.where(top, plan.Z + plan.T - 1, 0),
            )
        ]
    last = plan.T + plan.Z
    return [(0, 1, 0), (last, last, last + plan.T - 1)]


def corner_kernel(plan, *refs):
    n = len(refs) - 2
    zrecvs, outs = refs[:n], refs[n:]
    tiles = plan.corner_tiles()
    for out, to_next in zip(outs, plan.sides()):
        for k, zrecv in enumerate(zrecvs):

            def read(kind, i, h, row):
                return zrecv[i, h, pl.ds(row, 8), :]

            put_halo(plan, tiles, out, k * len(tiles), to_next, read)


def column_tiles(plan, parts):
    ahead = shift_left(plan, parts)
    tiles = []
    for h in range(plan.H):
        swapped = pltpu.roll(ahead[h], 4, 0)
        even = jnp.where(first_half(), parts[h], swapped)
        odd = jnp.where(first_half(), swapped, parts[h])
        high0 = even.astype(bf16).astype(f32)
        high1 = odd.astype(bf16).astype(f32)
        tiles.append(
            (
                jnp.concatenate([high0, even - high0], 0).astype(bf16),
                jnp.concatenate([high0, high1], 0).astype(bf16),
                jnp.concatenate([high1, odd - high1], 0).astype(bf16),
            )
        )
    return tiles


def put_columns(plan, columns, z, p, parts):
    for h, tiles in enumerate(column_tiles(plan, parts)):
        for j in range(3):
            columns[z, p, 16 * j : 16 * j + 16, h * LANES : (h + 1) * LANES] = tiles[j]


def shift_left(plan, parts):
    lane = lax.broadcasted_iota(jnp.int32, (8, LANES), 1)
    rolled = [pltpu.roll(p, LANES - 1, 1) for p in parts] + [jnp.zeros((8, LANES), f32)]
    return [jnp.where(lane == LANES - 1, rolled[h + 1], rolled[h]) for h in range(plan.H)]


def shift_right(plan, parts):
    lane = lax.broadcasted_iota(jnp.int32, (8, LANES), 1)
    rolled = [jnp.zeros((8, LANES), f32)] + [pltpu.roll(p, 1, 1) for p in parts]
    return [jnp.where(lane == 0, rolled[h], rolled[h + 1]) for h in range(plan.H)]


def prepare(plan, tables, U, V, DM, lam, mu, columns, z, pairs, level_rows):
    n_levels = tables.shape[0] // 2
    row = lax.broadcasted_iota(jnp.int32, (8, LANES), 0)
    spare = (row == 3) | (row == 7)
    for h in range(plan.H):
        for first in level_rows:
            level = U[z, h, pl.ds(4 * first + 3, 8, stride=4), :]
            dil = jnp.zeros((8, LANES), f32)
            she = jnp.zeros((8, LANES), f32)
            for k in range(n_levels):
                here = level == float(k + 1)
                dil = jnp.where(here, tables[k], dil)
                she = jnp.where(here, tables[n_levels + k], she)
            lam[z, h, first : first + 8, :] = dil
            mu[z, h, first : first + 8, :] = she
    for p in pairs:
        at = slice(8 * p, 8 * p + 8)
        for h in range(plan.H):
            v = V[z, h, at, :]
            mass = jnp.where(
                first_half(),
                jnp.broadcast_to(v[3:4, :], (8, LANES)),
                jnp.broadcast_to(v[7:8, :], (8, LANES)),
            )
            DM[z, h, at, :] = jnp.where(spare, 0.0, time_step * mass)
        put_columns(plan, columns, z, p, [U[z, h, at, :] for h in range(plan.H)])


def begin_kernel(plan, tables, xv, gown, *refs):
    n = len(refs) - 9
    zrecvs, firsts = refs[:n], refs[n : n + 2]
    U, V, DM, lam, mu, G, columns = refs[n + 2 :]
    Z, Y, X, H, T = plan.Z, plan.Y, plan.X, plan.H, plan.T
    PB, P0, R, ZB, ZS, YB = plan.PB, plan.P0, plan.hrow, plan.ZB, plan.ZS, plan.YB
    scal = place(plan)
    offset = scal[1]
    sides = plan.sides()
    mid = slice(R, R + 4 * Y)
    for z in range(Z):
        U[offset + z, :, mid, :] = xv[z, :, : 4 * Y, :]
        V[offset + z, :, mid, :] = xv[z, :, 4 * Y :, :]
    for zrecv, (at_u, at_v, lacks) in zip(zrecvs, halo_places(plan, scal)):
        for i in range(T):
            U[at_u + i, :, mid, :] = zrecv[i]
        for i in range(T - 1):
            V[at_v + i, :, mid, :] = zrecv[T + i]
        V[lacks, :, :, :] = jnp.zeros((H, 4 * YB, LANES), f32)
    for s in range(T):
        G[s] = jnp.zeros((H, 4 * YB, LANES), f32)
        G[s, :, mid, :] = gown[s]
    own, waves = plan.own_tiles()
    for source, from_next in zip(firsts, sides):

        def write(kind, z, h, row, tile):
            (U if kind == "u" else V)[offset + z, h, pl.ds(row, 8), :] = tile

        take_halo(plan, own, source, 0, from_next, write)
        for t, (s, h, k, n_pairs) in enumerate(waves):
            at = aligned(jnp.where(from_next, R + 4 * Y, R - 8 * n_pairs) + 8 * k)
            G[s, h, pl.ds(at, 8), :] = source[len(own) + t]

    def own_layer(z, carry):
        rows = [*range(0, YB - 7, 8), YB - 8]
        prepare(plan, tables, U, V, DM, lam, mu, columns, offset + z, range(PB), sorted(set(rows)))
        columns[offset + z, PB] = jnp.zeros((48, X), bf16)
        return carry

    lax.fori_loop(0, Z, own_layer, 0)
    for at_u, at_v, lacks in halo_places(plan, scal):

        def halo_layer(i, carry):
            rows = range(plan.hy, plan.hy + Y, 8)
            prepare(plan, tables, U, V, DM, lam, mu, columns, at_u + i, range(P0, P0 + Y // 2), rows)
            columns[at_u + i, PB] = jnp.zeros((48, X), bf16)
            return carry

        lax.fori_loop(0, T, halo_layer, 0)
    for z in range(ZB, ZS):
        for ref in (U, V, DM, lam, mu, columns):
            ref[z] = jnp.zeros(ref.shape[1:], ref.dtype)


def main_kernel(plan, tables, *refs):
    weights = refs[: len(VARIANTS)]
    corners = refs[len(VARIANTS) : len(refs) - 18]
    G = refs[len(refs) - 13]
    out_u, out_v, U, V, DM, lam, mu, columns, CI, F, spare_columns = refs[len(refs) - 11 :]
    Z, Y, X, H, T = plan.Z, plan.Y, plan.X, plan.H, plan.T
    PB, P0, R, ZB, ZS, YB = plan.PB, plan.P0, plan.hrow, plan.ZB, plan.ZS, plan.YB
    scal = place(plan)
    offset = scal[1]
    sides = plan.sides()
    halves = range(H)
    n_levels = tables.shape[0] // 2
    low_half = first_half()
    zero = jnp.zeros((8, LANES), f32)

    tiles = plan.corner_tiles()
    for k, (at_u, at_v, lacks) in enumerate(halo_places(plan, scal)):
        for source, from_next in zip(corners, sides):

            def write(kind, i, h, row, tile):
                if kind == "u":
                    U[at_u + i, h, pl.ds(row, 8), :] = tile
                else:
                    V[at_v + i - T, h, pl.ds(row, 8), :] = tile

            take_halo(plan, tiles, source, k * len(tiles), from_next, write)

        def halo_layer(i, carry):
            pairs = [*range(P0), *range(P0 + Y // 2, PB)]
            prepare(plan, tables, U, V, DM, lam, mu, columns, at_u + i, pairs, (0, YB - 8))
            return carry

        lax.fori_loop(0, T, halo_layer, 0)
    widest_pair = (plan.hy + Y + T - 2) // 2
    for z in range(ZS):
        for p in range(widest_pair + 1 if z < ZB else 0, PB + 1):
            spare_columns[z, p] = jnp.zeros((48, X), bf16)

    bottom = offset + Z - 1
    wave = tables[2 * n_levels]
    wave = jnp.where(scal[2] == 1, wave, zero)
    for h in halves:
        for p in range(PB):
            at = slice(8 * p, 8 * p + 8)
            CI[h, at, :] = wave * DM[bottom, h, at, :]

    def one_step(s, final):
        d = T - 1 - s
        cur, new = (columns, spare_columns)[:: 1 - 2 * (s % 2)]
        e_first, e_last = plan.hy - d - 1, plan.hy + Y - 1 + d
        p_first, p_last = e_first // 2, e_last // 2
        if plan.D == 1:
            first_z, n_z = 0, Z
        elif plan.swap:
            n_z = Z + d + 1
            first_z = jnp.where(scal[0] == 0, 0, ZB - n_z)
        else:
            first_z, n_z = T - d - 1, Z + 2 * d + 1
        single, count = n_z % 2, n_z // 2

        for p in range(p_first, p_last + 1):
            at = slice(8 * p, 8 * p + 8)
            for h in halves:
                v = V[bottom, h, at, :]
                V[bottom, h, at, :] = v + CI[h, at, :] * (G[s, h, at, :] - v)
        for p in range(p_first, p_last + 1):
            F[p] = jnp.zeros((2, H, 8, LANES), f32)

        def finish(z, p, g0, g1):
            at = slice(8 * p, 8 * p + 8)
            other = [
                pltpu.roll(jnp.where(low_half, g1[h], g0[h]), 4, 0) for h in halves
            ]
            other = shift_right(plan, other)
            fresh = []
            for h in halves:
                force = jnp.where(low_half, g0[h], g1[h]) + other[h]
                v = V[z, h, at, :] - DM[z, h, at, :] * force
                u = U[z, h, at, :] + time_step * v
                V[z, h, at, :] = v
                U[z, h, at, :] = u
                fresh.append(u)
            if not final:
                put_columns(plan, new, z, p, fresh)

        def layer_row(z0, n_layers):
            side = [[zero for _ in halves] for _ in range(n_layers + 1)]
            for p in range(p_first, p_last + 1):
                eys = tuple(ey for ey in range(2) if e_first <= 2 * p + ey <= e_last)
                kind = [(n, e) for n, e, _ in VARIANTS].index((n_layers, eys))
                pieces = []
                for zn in range(n_layers + 1):
                    start, stop = VARIANTS[kind][2]
                    pieces.append(cur[z0 + zn, p, start:48])
                    if stop > 48:
                        pieces.append(cur[z0 + zn, p + 1, : stop - 48])
                right = jnp.concatenate(pieces, 0)
                product = jnp.dot(weights[kind][...], right, preferred_element_type=f32)
                node = [[None] * 3 for _ in range(n_layers + 1)]
                for zn in range(n_layers + 1):
                    node[zn][0] = list(side[zn])
                for y in range(2):
                    above = [F[p, y, h] for h in halves]
                    node[0][y] = above if y else [a + b for a, b in zip(node[0][0], above)]
                for ez in range(n_layers):
                    for j, ey in enumerate(eys):
                        base = 64 * (len(eys) * ez + j)
                        y = 2 * p + ey
                        for h in halves:
                            lanes = slice(h * LANES, (h + 1) * LANES)
                            dil = jnp.broadcast_to(lam[z0 + ez, h, y : y + 1, :], (8, LANES))
                            she = jnp.broadcast_to(mu[z0 + ez, h, y : y + 1, :], (8, LANES))
                            for dz in range(2):
                                for dy in range(2):
                                    r = base + 8 * (2 * dz + dy)
                                    part = (
                                        dil * product[r : r + 8, lanes]
                                        + she * product[r + 32 : r + 40, lanes]
                                    )
                                    slot = node[ez + dz][ey + dy]
                                    if slot is None:
                                        slot = node[ez + dz][ey + dy] = [None] * H
                                    slot[h] = part if slot[h] is None else slot[h] + part
                for y in range(2):
                    for h in halves:
                        F[p, y, h] = node[n_layers][y][h]
                for zn in range(n_layers):
                    finish(z0 + zn, p, node[zn][0], node[zn][1])
                side = [node[zn][2] or [zero for _ in halves] for zn in range(n_layers + 1)]

        def rows(first, number, carry):
            for i in range(number):
                layer_row(first_z + single + 2 * (first + i), 2)
            return carry

        def whole_step(i, carry):
            if single:
                layer_row(first_z, 1)
            return rows(0, count, carry)

        if plan.ZB <= 16:
            lax.fori_loop(0, scal[3], whole_step, 0)
        else:
            if single:
                layer_row(first_z, 1)
            lax.fori_loop(0, count, lambda i, c: rows(i, 1, c), 0)

    for s in range(T):
        one_step(s, s == T - 1)

    for z in range(Z):
        for h in halves:
            lanes = slice(h * LANES, (h + 1) * LANES)
            for y in range(0, Y, 8):
                for c in range(3):
                    at = pl.ds(R + 4 * y + c, 8, stride=4)
                    out_u[c, z, y : y + 8, lanes] = U[offset + z, h, at, :]
                    out_v[c, z, y : y + 8, lanes] = V[offset + z, h, at, :]


def smem():
    return pl.BlockSpec(memory_space=pltpu.SMEM)


def vmem():
    return pl.BlockSpec(memory_space=pltpu.VMEM)


def per_device(plan, u, v, m, mat, dilation_table, shear_table, stiffness_pair, impedance, mask, inc):
    Z, Y, X, H, T, D, L = plan.Z, plan.Y, plan.X, plan.H, plan.T, plan.D, plan.L
    shape = lambda *dims: jax.ShapeDtypeStruct(dims, f32)

    room = pltpu.CompilerParams(vmem_limit_bytes=40 * 2**20)
    rows, cols = selectors()
    n_tables = 2 * dilation_table.shape[0] + 1
    made = pl.pallas_call(
        matrix_kernel,
        out_shape=[pltpu.VMEM((64 * part.shape[1], part.shape[3]), bf16) for part in cols]
        + [pltpu.VMEM((n_tables, 8, LANES), f32)],
        in_specs=[vmem()] * 2 + [smem()] * 3 + [vmem()] * len(cols),
        out_specs=[vmem()] * (len(cols) + 1),
        compiler_params=room,
        name="matrix",
    )(
        *[
            pltpu.with_memory_space_constraint(a, pltpu.HBM)
            for a in (
                stiffness_pair.reshape(48, 24),
                jnp.asarray(rows, bf16),
                dilation_table,
                shear_table,
                impedance,
                *[jnp.asarray(part, bf16) for part in cols],
            )
        ]
    )
    weights, tables = made[:-1], made[-1]

    n_sends = 0 if D == 1 else 1 if plan.swap else 2
    tiles, waves = plan.own_tiles()
    local = lambda *dims: pltpu.VMEM(dims, f32)
    edge = local(len(tiles) + len(waves), 8, LANES)
    packed = pl.pallas_call(
        lambda *refs: pack_kernel(plan, *refs),
        out_shape=[local(Z, H, 8 * Y, LANES), local(T, H, 4 * Y, LANES), edge, edge]
        + [local(2 * T - 1, H, 4 * Y, LANES)] * n_sends,
        in_specs=[vmem()] * 6,
        out_specs=[vmem()] * (4 + n_sends),
        compiler_params=room,
        name="pack",
    )(*[pltpu.with_memory_space_constraint(a, pltpu.HBM) for a in (u, v, m, mat, mask, inc)])
    xv, g, to_first, to_second = packed[:4]
    sends = packed[4:]

    def trade(array, start):
        pairs = [(i, i + 1) for i in range(start, L - 1, 2)]
        return lax.ppermute(array, "lat", pairs + [(j, i) for i, j in pairs])

    if D == 1:
        zrecvs = []
    elif plan.swap:
        zrecvs = [lax.ppermute(sends[0], "depth", [(0, 1), (1, 0)])]
    else:
        zrecvs = [
            lax.ppermute(sends[0], "depth", [(i, i + 1) for i in range(D - 1)]),
            lax.ppermute(sends[1], "depth", [(i + 1, i) for i in range(D - 1)]),
        ]
    firsts = [trade(to_first, 1), trade(to_second, 0)]
    corners = []
    if zrecvs:
        corner = local(len(zrecvs) * len(plan.corner_tiles()), 8, LANES)
        corner_first, corner_second = pl.pallas_call(
            lambda *refs: corner_kernel(plan, *refs),
            out_shape=[corner, corner],
            in_specs=[vmem()] * len(zrecvs),
            out_specs=[vmem()] * 2,
            compiler_params=room,
            name="corner",
        )(*[pltpu.with_memory_space_constraint(a, pltpu.VMEM) for a in zrecvs])
        corners = [trade(corner_first, 1), trade(corner_second, 0)]
    near = lambda arrays: [pltpu.with_memory_space_constraint(a, pltpu.VMEM) for a in arrays]
    grid = (plan.ZS, H, 4 * plan.YB, LANES)
    moduli = (plan.ZS, H, plan.YB, LANES)
    held = (plan.ZS, plan.PB + 1, 48, X)
    state = [local(*grid), local(*grid), local(*grid), local(*moduli), local(*moduli)]
    columns = pltpu.VMEM(held, bf16)
    begun = pl.pallas_call(
        lambda *refs: begin_kernel(plan, *refs),
        out_shape=[*state, local(T, H, 4 * plan.YB, LANES), columns],
        in_specs=[vmem()] * (5 + len(zrecvs)),
        out_specs=[vmem()] * 7,
        compiler_params=room,
        name="begin",
    )(*near([tables, xv, g, *zrecvs, *firsts]))
    *state_in, waves_in, columns_in = near(begun)
    n = 1 + len(weights) + len(corners)
    new_u, new_v, *_ = pl.pallas_call(
        lambda *refs: main_kernel(plan, *refs),
        out_shape=[shape(3, Z, Y, X), shape(3, Z, Y, X), *state, columns],
        in_specs=[vmem()] * (n + 7),
        out_specs=[vmem()] * 8,
        input_output_aliases={n + i: 2 + i for i in range(5)} | {n + 6: 7},
        scratch_shapes=[
            pltpu.VMEM((H, 4 * plan.YB, LANES), f32),
            pltpu.VMEM((plan.PB, 2, H, 8, LANES), f32),
            pltpu.VMEM(held, bf16),
        ],
        compiler_params=room,
        name="steps",
    )(*near([tables, *weights, *corners]), *state_in, waves_in, columns_in)
    return new_u, new_v


def solution(mesh):
    field = P(None, "depth", "lat", None)
    in_specs = (
        field,
        field,
        P("depth", "lat", None),
        P("depth", "lat", None),
        P(),
        P(),
        P(),
        P(),
        P("lat", None),
        P(None, None, "lat", None),
    )

    def whole(displacement, *rest):
        plan = Plan(mesh, displacement, rest[-1])
        return jax.shard_map(
            lambda *args: per_device(plan, *args),
            mesh=mesh,
            in_specs=in_specs,
            out_specs=(field, field),
            check_vma=False,
        )(displacement, *rest)

    return whole
```
